256 devices in a mesh: ba: 8 (over x, core), ma: 16 (over z, y_hi), row: 2 (over y_lo).
Axes of the slice: x: 4, y: 4 (y_hi: 2, y_lo: 2; y = y_hi * 2 + y_lo), z: 8, core: 2. Of those that a mesh axis runs over, the one named last changes fastest.
Arguments:
- tokens: bfloat16 [16, 256, 4096], P(('ba', 'row'), None, 'ma'), may hold values from -6 to 6
- attn_gain: bfloat16 [4096], P('ma'), may hold values from 0.25 to 1.75
- query_weight: bfloat16 [4096, 4096], P('row', 'ma'), may hold values from -0.046875 to 0.046875
- key_weight: bfloat16 [4096, 4096], P('row', 'ma'), may hold values from -0.046875 to 0.046875
- value_projection_matrix: bfloat16 [4096, 4096], P('row', 'ma'), may hold values from -0.09375 to 0.09375
- attention_output_matrix: bfloat16 [4096, 4096], P('ma', 'row'), may hold values from -0.125 to 0.125
- bucket_bias_matrix: float32 [32, 64], P(None, 'ma'), may hold values from -6 to 215, as said below
- ffn_gain: bfloat16 [4096], P('ma'), may hold values from 0.25 to 1.75
- gate_weight: bfloat16 [4096, 8192], P(None, ('ma', 'row')), may hold values from -0.09375 to 0.09375
- up_weight: bfloat16 [4096, 8192], P(None, ('ma', 'row')), may hold values from -0.09375 to 0.09375
- down_projection_weight: bfloat16 [8192, 4096], P(('ma', 'row')), may hold values from -0.125 to 0.125
Outputs:
- encoded: bfloat16 [16, 256, 4096], P(('ba', 'row'), None, 'ma')
The draws below stay inside these ranges and needn't reach their ends.
Inputs may be any that keep to these rules, and one draw needn't show every extreme that they name: `bucket_bias_matrix`: entries of the relative position table.
All inputs are finite; a program needn't handle non-finite values.
Results may differ from the reference program's by a relative error of at most 0.017.
Values may be sent and summed in bfloat16 or wider, within the bound.
No kernel may reach another device: no remote copies, remote signals or barrier semaphores. Data moves between devices by JAX's collectives and lax.ppermute only.
A program may use at most 128 MiB of HBM per device.

```python
import jax
import jax.numpy as jnp
from jax import lax

D = 4096
H = 64
DH = 64
FF = 8192
BUCKETS = 32
LEN = 256
BATCH = 16
N_MA = 16


def draw_bucket_bias_matrix(key, part):
    first_key, second_key = jax.random.split(key)
    normal_part = jnp.clip(jax.random.normal(first_key, (BUCKETS, H), jnp.float32), -6.0, 6.0)
    return normal_part


def spiked(entries, own_key, source, target, shards_of, factor):
    owner, partner = [(jnp.arange(entries.shape[axis_at]) // (entries.shape[axis_at] // shards_of)).reshape([-1 if axis == axis_at else 1 for axis in range(entries.ndim)]) for axis_at in (source, target)]
    chosen = jax.random.permutation(own_key, shards_of)[partner]
    strong = (owner == chosen) | (owner == (partner + shards_of // 2) % shards_of)
    return jnp.where(strong, factor * entries, entries)


def steps_of(stream_key, shape, cuts, smallest, largest):
    def one(position, shards_of):
        heights = jax.random.uniform(jax.random.fold_in(jax.random.fold_in(stream_key, 6), position), (shards_of,), jnp.float32, smallest / len(cuts), largest / len(cuts))
        return jnp.repeat(jnp.exp(heights), shape[position] // shards_of).reshape((-1,) + (1,) * (len(shape) - position - 1))

    loudness = one(*cuts[0])
    for cut in cuts[1:]:
        loudness = loudness * one(*cut)
    return loudness


def noise(stream_key, extent, spread, limit, cuts=(), held_as=jnp.bfloat16):
    loudness = steps_of(stream_key, extent, cuts, -0.22, 0.18) if cuts else 1.0
    entries = jax.random.normal(stream_key, extent, jnp.float32) * spread * loudness
    return jnp.minimum(jnp.maximum(entries, -limit), limit).astype(held_as)


def noise_with(rng, dims, deviation, most, pieces, heavy, kind=jnp.bfloat16):
    result = deviation * jax.random.normal(rng, dims, jnp.float32)
    if pieces:
        result = result * steps_of(rng, dims, pieces, -0.22, 0.18)
    return jnp.clip(spiked(result, jax.random.fold_in(rng, 3), *heavy), -most, most).astype(kind)


def setup_inputs(seed: int = 0) -> dict:
    key_of = jax.random.split(jax.random.key(seed), 12)
    tokens = noise(key_of[0], (BATCH, LEN, D), 1.0, 6.0, ((0, 16), (2, 16)))
    attn_gain = jnp.clip(1.0 + 0.15 * jax.random.normal(key_of[1], (D,), jnp.float32), 0.25, 1.75).astype(jnp.bfloat16)
    query_weight = noise(key_of[2], (D, H * DH), (4 * D) ** -0.5, 0.046875, ((0, 2), (1, 16)))
    key_weight = noise(key_of[3], (D, H * DH), (4 * D) ** -0.5, 0.046875, ((0, 2), (1, 16)))
    value_projection_matrix = noise(key_of[4], (D, H * DH), D ** -0.5, 0.09375, ((0, 2), (1, 16)))
    attention_output_matrix = noise_with(key_of[5], (H * DH, D), (H * DH) ** -0.5, 0.125, ((0, 16), (1, 2)), (0, 1, 16, 2.0))
    bucket_bias_matrix = draw_bucket_bias_matrix(jax.random.fold_in(key_of[11], 71), 0)
    ffn_gain = jnp.clip(1.0 + 0.15 * jax.random.normal(key_of[7], (D,), jnp.float32), 0.25, 1.75).astype(jnp.bfloat16)
    gate_weight = noise(key_of[8], (D, FF), D ** -0.5, 0.09375, ((1, 32),))
    up_weight = noise(key_of[9], (D, FF), D ** -0.5, 0.09375, ((1, 32),))
    down_projection_weight = noise_with(key_of[10], (FF, D), FF ** -0.5, 0.125, ((0, 32),), (0, 1, 32, 2.75))
    return dict(tokens=tokens, attn_gain=attn_gain, query_weight=query_weight, key_weight=key_weight, value_projection_matrix=value_projection_matrix, attention_output_matrix=attention_output_matrix, bucket_bias_matrix=bucket_bias_matrix, ffn_gain=ffn_gain, gate_weight=gate_weight, up_weight=up_weight, down_projection_weight=down_projection_weight)


bucket_thresholds = (1, 2, 3, 4, 5, 6, 7, 8, 11, 16, 23, 32, 45, 64, 91, 128)
epsilon = 1e-06

def buckets(length):
    places = jnp.arange(length, dtype=jnp.int32)
    offset = places[None, :] - places[:, None]
    distance = jnp.abs(offset)
    backward = jnp.zeros_like(distance)
    for threshold in bucket_thresholds[:15]:
        backward = backward + (distance >= threshold).astype(jnp.int32)
    forward = jnp.full_like(distance, 15)
    for threshold in bucket_thresholds:
        forward = forward + (distance >= threshold).astype(jnp.int32)
    return jnp.where(offset > 0, forward, backward)

def rms_scale(values, gain):
    mean_square = lax.optimization_barrier(jnp.mean(values * values, axis=-1, keepdims=True))
    return (values * lax.rsqrt(mean_square + epsilon) * gain.astype(jnp.float32)).astype(jnp.bfloat16)

def grouped_sum(left, right, groups):
    span = left.shape[1] // groups

    def add_group(running, group_index):
        columns = lax.dynamic_slice_in_dim(left, group_index * span, span, 1)
        matrix = lax.dynamic_slice_in_dim(right, group_index * span, span, 0)
        partial_term = jnp.dot(columns, matrix, preferred_element_type=jnp.float32).astype(jnp.bfloat16)
        partial_term = lax.optimization_barrier(partial_term).astype(jnp.float32)
        return (running + partial_term, None)
    start_sum = jnp.zeros((left.shape[0], right.shape[1]), jnp.float32)
    total, unused = lax.scan(add_group, start_sum, jnp.arange(groups, dtype=jnp.int32))
    return total

def reference(tokens, attn_gain, query_weight, key_weight, value_projection_matrix, attention_output_matrix, bucket_bias_matrix, ffn_gain, gate_weight, up_weight, down_projection_weight):
    batch_size, length, model_width = tokens.shape
    head_count = bucket_bias_matrix.shape[1]
    inner_width = query_weight.shape[1]
    head_size = inner_width // head_count
    token_rows = tokens.reshape(batch_size * length, model_width).astype(jnp.float32)
    normed = rms_scale(token_rows, attn_gain)
    projected = tuple((jnp.dot(normed, matrix, preferred_element_type=jnp.float32).astype(jnp.bfloat16).reshape(batch_size, length, head_count, head_size) for matrix in (query_weight, key_weight, value_projection_matrix)))
    relative_position_scores = jnp.transpose(bucket_bias_matrix[buckets(length)], (2, 0, 1))

    def attend(inputs):
        query_heads, key_heads, value_heads = inputs
        scores = jnp.einsum('qhd,khd->hqk', query_heads.astype(jnp.float32), key_heads.astype(jnp.float32)) + relative_position_scores
        row_max = lax.optimization_barrier(jnp.max(scores, axis=-1, keepdims=True))
        exponent = jnp.exp(scores - row_max)
        weights = (exponent / lax.optimization_barrier(jnp.sum(exponent, axis=-1, keepdims=True))).astype(jnp.bfloat16)
        return jnp.einsum('hqk,khd->qhd', weights.astype(jnp.float32), value_heads.astype(jnp.float32)).astype(jnp.bfloat16)
    attended = lax.map(attend, projected).reshape(batch_size * length, inner_width)
    attn_out = grouped_sum(attended, attention_output_matrix, N_MA)
    residual_stream = (token_rows + attn_out).astype(jnp.bfloat16)
    residual_f = residual_stream.astype(jnp.float32)
    ffn_in = rms_scale(residual_f, ffn_gain)
    gate_act = jnp.dot(ffn_in, gate_weight, preferred_element_type=jnp.float32)
    up_act = jnp.dot(ffn_in, up_weight, preferred_element_type=jnp.float32)
    hidden = (jax.nn.gelu(gate_act, approximate=True) * up_act).astype(jnp.bfloat16)
    ffn_out = jnp.dot(hidden, down_projection_weight, preferred_element_type=jnp.float32)
    encoded = (residual_f + ffn_out).astype(jnp.bfloat16)
    return encoded.reshape(batch_size, length, model_width)
```

```python
import jax
import jax.numpy as jnp
from jax import lax
from jax.sharding import Mesh
from jax.sharding import PartitionSpec as P

MA = ("ma_0", "ma_1")
MA_ROW = ("ma_0", "ma_1", "row")

bucket_thresholds = (1, 2, 3, 4, 5, 6, 7, 8, 11, 16, 23, 32, 45, 64, 91, 128)
epsilon = 1e-06
RING = 8
SWAP = [(0, 1), (1, 0)]
UP = [(i, (i + 1) % RING) for i in range(RING)]
DOWN = [(i, (i - 1) % RING) for i in range(RING)]


def buckets(length):
    places = jnp.arange(length, dtype=jnp.int32)
    offset = places[None, :] - places[:, None]
    distance = jnp.abs(offset)
    backward = jnp.zeros_like(distance)
    for threshold in bucket_thresholds[:15]:
        backward = backward + (distance >= threshold).astype(jnp.int32)
    forward = jnp.full_like(distance, 15)
    for threshold in bucket_thresholds:
        forward = forward + (distance >= threshold).astype(jnp.int32)
    return jnp.where(offset > 0, forward, backward)


def tied(value, *after):
    return lax.optimization_barrier((value, *after))[0]


def pair_order(mine, theirs, axis):
    first = lax.axis_index("ma_1") == 0
    return jnp.where(
        first,
        jnp.concatenate([mine, theirs], axis=axis),
        jnp.concatenate([theirs, mine], axis=axis),
    )


def ring_gather(block):
    held = {0: block}
    above = below = block
    for step in range(1, RING // 2 + 1):
        above = lax.ppermute(above, "ma_0", DOWN)
        held[step] = above
        if step < RING // 2:
            below = lax.ppermute(below, "ma_0", UP)
            held[RING - step] = below
    return held


def ring_sum(block_for):
    up = block_for(4).astype(jnp.bfloat16)
    down = None
    for step in range(1, RING // 2 + 1):
        got_up = lax.ppermute(up, "ma_0", UP)
        if step == 1:
            down = block_for(-3).astype(jnp.bfloat16)
            got_down = None
        else:
            got_down = lax.ppermute(down, "ma_0", DOWN)
        if step < RING // 2:
            up = (got_up.astype(jnp.float32) + block_for(4 - step)).astype(jnp.bfloat16)
            if got_down is not None:
                down = (got_down.astype(jnp.float32) + block_for(step - 4)).astype(jnp.bfloat16)
    return got_up.astype(jnp.float32) + got_down.astype(jnp.float32) + block_for(0)


def place(ring_at, half, owner):
    at = jnp.mod(ring_at + owner, RING)
    return jnp.mod(at + half * (RING // 2), RING)


def spread(values, gain, ring_at, half):
    rows, width = values.shape
    as_float = values.astype(jnp.float32)
    squares = jnp.sum(as_float * as_float, axis=1)
    gained = (as_float * gain.astype(jnp.float32)).astype(jnp.bfloat16)
    tail = jnp.zeros((8, width), jnp.bfloat16).at[0, :rows].set(squares.astype(jnp.bfloat16))
    held = ring_gather(jnp.concatenate([gained, tail], axis=0))
    buffer = jnp.zeros((rows, width * RING), jnp.bfloat16)
    total = jnp.zeros((rows,), jnp.float32)
    for owner in (0, 1, 7, 2, 6, 3, 5, 4):
        block = held[owner]
        slot = place(ring_at, half, owner)
        buffer = lax.dynamic_update_slice(buffer, block[:rows], (0, slot * width))
        total = total + block[rows, :rows].astype(jnp.float32)
    scale = lax.rsqrt(total / (width * RING) + epsilon)
    return buffer, scale[:, None]


def on_device(
    tokens,
    attn_gain,
    query_weight,
    key_weight,
    value_projection_matrix,
    attention_output_matrix,
    bucket_bias_matrix,
    ffn_gain,
    gate_weight,
    up_weight,
    down_projection_weight,
):
    sequences, length, part = tokens.shape
    local_heads = bucket_bias_matrix.shape[1]
    inner = query_weight.shape[1]
    head_size = inner // local_heads
    half = lax.axis_index("row")
    ring_at = lax.axis_index("ma_0")
    copy_at = lax.axis_index("ba")
    copies = lax.axis_size("ba")
    token_rows = tokens.reshape(length, part)

    gains = jnp.concatenate(
        [attn_gain[None], ffn_gain[None], jnp.zeros((6, part), jnp.bfloat16)], axis=0
    )
    mine = jnp.concatenate([token_rows, gains], axis=0)
    theirs = lax.ppermute(mine, "ma_1", SWAP)

    half_rows = query_weight.shape[0]
    depth = half_rows // copies
    share = [
        lax.dynamic_slice_in_dim(w, copy_at * depth, depth, 0)
        for w in (query_weight, key_weight, value_projection_matrix)
    ]
    out_width = attention_output_matrix.shape[1] // copies
    share.append(
        lax.dynamic_slice_in_dim(attention_output_matrix, copy_at * out_width, out_width, 1)
    )
    first_share = lax.ppermute(jnp.concatenate(share, axis=1), "row", SWAP)
    other_first = lax.all_gather(first_share, "ba", axis=0, tiled=True)

    gate_depth = gate_weight.shape[0] // copies
    gate_share = [
        lax.dynamic_slice_in_dim(w, copy_at * gate_depth, gate_depth, 0)
        for w in (gate_weight, up_weight)
    ]
    down_width = down_projection_weight.shape[1] // copies
    down_share = lax.dynamic_slice_in_dim(
        down_projection_weight, copy_at * down_width, down_width, 1
    )
    second_share = jnp.concatenate([jnp.concatenate(gate_share, axis=1), down_share], axis=0)
    second_share = tied(second_share, theirs)
    second_share = lax.ppermute(second_share, "row", SWAP)
    second_share = tied(second_share, other_first)
    other_second = lax.all_gather(second_share, "ba", axis=0, tiled=False)

    wide = pair_order(mine, theirs, 1)
    wide_tokens = wide[:length]
    wide_attn_gain = wide[length]
    wide_ffn_gain = wide[length + 1]

    gained, scale = spread(wide_tokens, wide_attn_gain, ring_at, half)
    own_part, other_part = gained[:, :half_rows], gained[:, half_rows:]
    projected = []
    for k, w in enumerate((query_weight, key_weight, value_projection_matrix)):
        product = jnp.dot(own_part, w, preferred_element_type=jnp.float32)
        product = product + jnp.dot(
            other_part,
            other_first[:, k * inner : (k + 1) * inner],
            preferred_element_type=jnp.float32,
        )
        projected.append((product * scale).astype(jnp.bfloat16))
    query_heads, key_heads, value_heads = [
        member.reshape(length, local_heads, head_size) for member in projected
    ]
    bucket_grid = buckets(length)
    table_rows = jnp.arange(bucket_bias_matrix.shape[0], dtype=jnp.int32)
    bucket_indicator = (table_rows[:, None, None] == bucket_grid[None, :, :]).astype(jnp.float32)
    relative_position_scores = jnp.einsum(
        "dmy,du->umy", bucket_indicator, bucket_bias_matrix, precision=lax.Precision.HIGHEST
    )
    scores = (
        jnp.einsum("qhd,khd->hqk", query_heads, key_heads, preferred_element_type=jnp.float32)
        + relative_position_scores
    )
    row_max = jnp.max(scores, axis=-1, keepdims=True)
    exponent = jnp.exp(scores - row_max)
    weights = (exponent / jnp.sum(exponent, axis=-1, keepdims=True)).astype(jnp.bfloat16)
    attended = jnp.einsum("hqk,khd->qhd", weights, value_heads, preferred_element_type=jnp.float32)
    attended = attended.astype(jnp.bfloat16).reshape(length, inner)

    own_out = jnp.einsum(
        "tf,fmd->mtd",
        attended,
        attention_output_matrix.reshape(inner, copies, out_width),
        preferred_element_type=jnp.float32,
    )
    other_out = jnp.einsum(
        "tf,mfd->mtd",
        attended,
        other_first[:, 3 * inner :].reshape(copies, inner, out_width),
        preferred_element_type=jnp.float32,
    )
    both_out = jnp.concatenate([own_out, other_out], axis=0).astype(jnp.bfloat16)
    both_out = both_out.reshape(RING, 2, length, out_width)

    def out_block(owner):
        slot = place(ring_at, half, owner)
        return lax.dynamic_index_in_dim(both_out, slot, 0, keepdims=False).astype(jnp.float32)

    summed = ring_sum(out_block).astype(jnp.bfloat16)
    partner = lax.ppermute(summed, "ma_1", SWAP)
    attn_out = summed.astype(jnp.float32) + partner.astype(jnp.float32)
    attn_out = jnp.concatenate([attn_out[0], attn_out[1]], axis=1)
    residual = (wide_tokens.astype(jnp.float32) + attn_out).astype(jnp.bfloat16)
    first = lax.axis_index("ma_1") == 0
    own_residual = jnp.where(first, residual[:, :part], residual[:, part:])

    gained, scale = spread(residual, wide_ffn_gain, ring_at, jnp.zeros_like(half))
    hidden_terms = []
    other_gate = other_second[:, :gate_depth, :inner].reshape(-1, inner)
    other_up = other_second[:, :gate_depth, inner:].reshape(-1, inner)
    for gate, up in ((gate_weight, up_weight), (other_gate, other_up)):
        gate_act = jnp.dot(gained, gate, preferred_element_type=jnp.float32) * scale
        up_act = jnp.dot(gained, up, preferred_element_type=jnp.float32) * scale
        hidden_terms.append((jax.nn.gelu(gate_act, approximate=True) * up_act).astype(jnp.bfloat16))
    down_out = jnp.einsum(
        "tf,fmd->mtd",
        hidden_terms[0],
        down_projection_weight.reshape(-1, copies, down_width),
        preferred_element_type=jnp.float32,
    ) + jnp.einsum(
        "tf,mfd->mtd",
        hidden_terms[1],
        other_second[:, gate_depth:],
        preferred_element_type=jnp.float32,
    )
    down_out = down_out.astype(jnp.bfloat16)

    def down_block(owner):
        slot = jnp.mod(ring_at + owner, RING)
        return lax.dynamic_index_in_dim(down_out, slot, 0, keepdims=False).astype(jnp.float32)

    summed = ring_sum(down_block)
    low, high = summed[:, :part], summed[:, part:]
    keep = jnp.where(first, low, high)
    give = jnp.where(first, high, low).astype(jnp.bfloat16)
    got = lax.ppermute(give, "ma_1", SWAP)
    encoded = own_residual.astype(jnp.float32) + keep + got.astype(jnp.float32)
    return encoded.astype(jnp.bfloat16).reshape(sequences, length, part)


def solution(mesh):
    split = Mesh(
        mesh.devices.reshape(mesh.shape["ba"], RING, 2, mesh.shape["row"]),
        ("ba", "ma_0", "ma_1", "row"),
    )
    return jax.shard_map(
        on_device,
        mesh=split,
        in_specs=(
            P(("ba", "row"), None, MA),
            P(MA),
            P("row", MA),
            P("row", MA),
            P("row", MA),
            P(MA, "row"),
            P(None, MA),
            P(MA),
            P(None, MA_ROW),
            P(None, MA_ROW),
            P(MA_ROW, None),
        ),
        out_specs=P(("ba", "row"), None, MA),
        check_vma=False,
    )
```

```python
import functools

import jax
import jax.numpy as jnp
from jax import lax
from jax.experimental import pallas as pl
from jax.experimental.pallas import tpu as pltpu
from jax.sharding import Mesh
from jax.sharding import PartitionSpec as P

MA = ("ma_0", "ma_1")
MA_ROW = ("ma_0", "ma_1", "row")

bucket_thresholds = (1, 2, 3, 4, 5, 6, 7, 8, 11, 16, 23, 32, 45, 64, 91, 128)
epsilon = 1e-06
RING = 8
SWAP = [(0, 1), (1, 0)]
UP = [(i, (i + 1) % RING) for i in range(RING)]
DOWN = [(i, (i - 1) % RING) for i in range(RING)]


def tied(value, *after):
    return lax.optimization_barrier((value, *after))[0]


def pair_order(mine, theirs, axis):
    first = lax.axis_index("ma_1") == 0
    return jnp.where(
        first,
        jnp.concatenate([mine, theirs], axis=axis),
        jnp.concatenate([theirs, mine], axis=axis),
    )


def ring_gather(block):
    held = {0: block}
    above = below = block
    for step in range(1, RING // 2 + 1):
        above = lax.ppermute(above, "ma_0", DOWN)
        held[step] = above
        if step < RING // 2:
            below = lax.ppermute(below, "ma_0", UP)
            held[RING - step] = below
    return held


SEND = (4, 5, 3, 6, 2, 7, 1, 0)


def ring_sum(stack):
    def block(owner):
        return stack[SEND.index(owner % RING)].astype(jnp.float32)

    up, down = stack[0], stack[1]
    got_down = None
    for step in range(1, RING // 2 + 1):
        got_up = lax.ppermute(up, "ma_0", UP)
        if step > 1:
            got_down = lax.ppermute(down, "ma_0", DOWN)
        if step < RING // 2:
            up = (got_up.astype(jnp.float32) + block(4 - step)).astype(jnp.bfloat16)
            if got_down is not None:
                down = (got_down.astype(jnp.float32) + block(step - 4)).astype(jnp.bfloat16)
    return got_up.astype(jnp.float32) + got_down.astype(jnp.float32) + block(0)


VMEM = pltpu.MemorySpace.VMEM


def whole(shape):
    zeros = (0,) * len(shape)
    return pl.BlockSpec(shape, lambda *_: zeros)


def bias_kernel(bucket_ref, table_ref, bias_ref):
    heads, rows, columns = bias_ref.shape
    row = bucket_ref[0:1, :]
    for h in range(heads):
        line = jnp.zeros(row.shape, jnp.float32)
        for b in range(table_ref.shape[0]):
            line = jnp.where(row == b, table_ref[b : b + 1, h : h + 1], line)
        wide = jnp.broadcast_to(line, (rows, row.shape[1]))
        bias_ref[h] = pltpu.roll(wide, 0, 1, stride=1, stride_axis=0)[:, :columns]


def position_bias(table, length):
    offset = jnp.arange(2 * length, dtype=jnp.int32)
    offset = jnp.where(offset < length, offset, offset - 2 * length)
    distance = jnp.abs(offset)
    bucket = jnp.where(offset > 0, 15, 0)
    for threshold in bucket_thresholds[:15]:
        bucket = bucket + (distance >= threshold).astype(jnp.int32)
    last = (distance >= bucket_thresholds[15]) & (offset > 0)
    bucket = bucket + last.astype(jnp.int32)
    heads = table.shape[1]
    return pl.pallas_call(
        bias_kernel,
        out_shape=jax.ShapeDtypeStruct((heads, length, length), jnp.float32),
        cost_estimate=pl.CostEstimate(flops=10**8, bytes_accessed=10**6, transcendentals=0),
        name="position_bias",
    )(jnp.broadcast_to(bucket[None], (8, 2 * length)), table)


def pick(step, block_refs, held_ref):
    for k, ref in enumerate(block_refs):

        @pl.when(step == k)
        def _(ref=ref):
            held_ref[...] = ref[...]


def as_column(line):
    size = line.shape[1]
    at_row = lax.broadcasted_iota(jnp.int32, (size, size), 0)
    at_column = lax.broadcasted_iota(jnp.int32, (size, size), 1)
    spread_out = jnp.where(at_row == at_column, jnp.broadcast_to(line, (size, size)), 0.0)
    return jnp.sum(spread_out, axis=1, keepdims=True)


def dot(a, b):
    return jnp.dot(a, b, preferred_element_type=jnp.float32)


def attention_kernel(width, at_ref, *refs):
    blocks = refs[:RING]
    own = refs[RING : RING + 3]
    other = refs[RING + 3 : RING + 6]
    own_out_ref, other_out_ref, bias_ref = refs[RING + 6 : RING + 9]
    out_ref, held_ref, acc_ref, squares_ref, attended_ref = refs[RING + 9 :]
    step = pl.program_id(0)
    length = acc_ref.shape[0]
    inner = attended_ref.shape[1]

    @pl.when(step == 0)
    def _():
        acc_ref[...] = jnp.zeros_like(acc_ref)
        squares_ref[...] = jnp.zeros_like(squares_ref)

    @pl.when(step < RING)
    def _():
        pick(step, blocks, held_ref)
        squares_ref[...] += held_ref[length : length + 8, :length].astype(jnp.float32)
        rows = held_ref[:length, :]

        def add(weights):
            for k, w in enumerate(weights):
                acc_ref[:, k * inner : (k + 1) * inner] += dot(rows, w[...])

        mine = at_ref[2, step] == 1

        @pl.when(mine)
        def _():
            add(own)

        @pl.when(jnp.logical_not(mine))
        def _():
            add(other)

    @pl.when(step == RING)
    def _():
        mean = squares_ref[0:1, :] / width
        scale = as_column(lax.rsqrt(mean + epsilon))
        query, key, value = (
            (acc_ref[:, k * inner : (k + 1) * inner] * scale).astype(jnp.bfloat16) for k in range(3)
        )
        heads = bias_ref.shape[0]
        size = inner // heads
        for h in range(heads):
            at = slice(h * size, (h + 1) * size)
            scores = lax.dot_general(
                query[:, at], key[:, at], (((1,), (1,)), ((), ())),
                preferred_element_type=jnp.float32,
            ) + bias_ref[h]
            exponent = jnp.exp(scores - jnp.max(scores, axis=-1, keepdims=True))
            weights = exponent / jnp.sum(exponent, axis=-1, keepdims=True)
            attended_ref[:, at] = dot(weights.astype(jnp.bfloat16), value[:, at]).astype(
                jnp.bfloat16
            )

    @pl.when(step >= RING)
    def _():
        attended = attended_ref[...]
        mine = at_ref[5, step] == 1

        @pl.when(mine)
        def _():
            out_ref[0] = dot(attended, own_out_ref[...]).astype(jnp.bfloat16)

        @pl.when(jnp.logical_not(mine))
        def _():
            for k in range(2):
                part = other_out_ref[k * inner : (k + 1) * inner, :]
                out_ref[0, :, k * inner : (k + 1) * inner] = dot(attended, part).astype(
                    jnp.bfloat16
                )


def held_index(wanted, use):
    out = []
    last = wanted[-1]
    for w, u in zip(reversed(wanted), reversed(use)):
        last = jnp.where(u, w, last)
    for w, u in zip(wanted, use):
        last = jnp.where(u, w, last)
        out.append(last)
    return out


def attention(held, bias, own, other_first, own_out, ring_at, half):
    length = bias.shape[1]
    inner = own[0].shape[1]
    rows, wide = held[0].shape
    depth = wide

    def slots(owners):
        where = [jnp.mod(jnp.mod(ring_at + k, RING) + half * (RING // 2), RING) for k in owners]
        mine = [s < RING // 2 for s in where]
        theirs = [jnp.logical_not(m) for m in mine]
        return (
            held_index([jnp.minimum(s, RING // 2 - 1) for s in where], mine),
            held_index([jnp.maximum(s - RING // 2, 0) for s in where], theirs),
            [m.astype(jnp.int32) for m in mine],
        )

    first = slots(range(RING))
    second = slots(SEND)
    table = jnp.stack(
        [jnp.stack([jnp.asarray(v, jnp.int32) for v in line + line2])
         for line, line2 in [(f, [f[-1]] * RING) for f in first]
         + [([s[0]] * RING, s) for s in second]]
    )
    grid = 2 * RING

    return pl.pallas_call(
        functools.partial(attention_kernel, float(wide * RING)),
        grid_spec=pltpu.PrefetchScalarGridSpec(
            num_scalar_prefetch=1,
            grid=(grid,),
            in_specs=[whole((rows, wide))] * RING
            + [pl.BlockSpec((depth, inner), lambda i, at: (at[0, i], 0))] * 3
            + [
                pl.BlockSpec((depth, inner), functools.partial(lambda k, i, at: (at[1, i], k), k))
                for k in range(3)
            ]
            + [
                pl.BlockSpec((inner, wide), lambda i, at: (0, at[3, i])),
                pl.BlockSpec((2 * inner, inner), lambda i, at: (at[4, i], 3)),
                whole(bias.shape),
            ],
            out_specs=pl.BlockSpec((1, length, wide), lambda i, at: (jnp.maximum(i - RING, 0), 0, 0)),
            scratch_shapes=[
                pltpu.VMEM((rows, wide), jnp.bfloat16),
                pltpu.VMEM((length, 3 * inner), jnp.float32),
                pltpu.VMEM((8, length), jnp.float32),
                pltpu.VMEM((length, inner), jnp.bfloat16),
            ],
        ),
        out_shape=jax.ShapeDtypeStruct((RING, length, wide), jnp.bfloat16),
        cost_estimate=pl.CostEstimate(
            flops=2 * length * wide * RING * 4 * inner, bytes_accessed=10**7, transcendentals=0
        ),
        name="attention",
    )(
        table,
        *[held[k] for k in range(RING)],
        *own,
        other_first,
        other_first,
        other_first,
        own_out,
        other_first,
        bias,
    )


EARLY = (0, 1, 7, 2, 6)
LATE = (3, 5, 4)


def gate_steps(step, count, blocks, gate_ref, up_ref, other_ref, held_ref, acc_ref, squares_ref):
    length = acc_ref.shape[0]
    hidden = gate_ref.shape[1]

    @pl.when(step < count)
    def _():
        pick(step, blocks, held_ref)
        squares_ref[...] += held_ref[length : length + 8, :length].astype(jnp.float32)
        rows = held_ref[:length, :]
        acc_ref[:, :hidden] += dot(rows, gate_ref[...])
        acc_ref[:, hidden : 2 * hidden] += dot(rows, up_ref[...])
        acc_ref[:, 2 * hidden :] += dot(rows, other_ref[0])


def gate_kernel(at_ref, *refs):
    count = len(EARLY)
    blocks = refs[:count]
    gate_ref, up_ref, other_ref = refs[count : count + 3]
    acc_ref, squares_ref, held_ref = refs[count + 3 :]
    step = pl.program_id(0)

    @pl.when(step == 0)
    def _():
        acc_ref[...] = jnp.zeros_like(acc_ref)
        squares_ref[...] = jnp.zeros_like(squares_ref)

    gate_steps(step, count, blocks, gate_ref, up_ref, other_ref, held_ref, acc_ref, squares_ref)


def down_kernel(width, at_ref, *refs):
    count = len(LATE)
    blocks = refs[:count]
    gate_ref, up_ref, other_ref, acc_in_ref, squares_in_ref = refs[count : count + 5]
    down_ref, other_down_ref = refs[count + 5 : count + 7]
    out_ref, held_ref, acc_ref, squares_ref, hidden_ref = refs[count + 7 :]
    step = pl.program_id(0)

    @pl.when(step == 0)
    def _():
        acc_ref[...] = acc_in_ref[...]
        squares_ref[...] = squares_in_ref[...]

    gate_steps(step, count, blocks, gate_ref, up_ref, other_ref, held_ref, acc_ref, squares_ref)
    size = gate_ref.shape[1]

    @pl.when(step == count)
    def _():
        mean = squares_ref[0:1, :] / width
        scale = as_column(lax.rsqrt(mean + epsilon))
        for k in range(2):
            gate = acc_ref[:, 2 * k * size : (2 * k + 1) * size] * scale
            up = acc_ref[:, (2 * k + 1) * size : (2 * k + 2) * size] * scale
            hidden_ref[:, k * size : (k + 1) * size] = (
                jax.nn.gelu(gate, approximate=True) * up
            ).astype(jnp.bfloat16)

    @pl.when(step >= count)
    def _():
        out_ref[0] = (
            dot(hidden_ref[:, :size], down_ref[...]) + dot(hidden_ref[:, size:], other_down_ref[0])
        ).astype(jnp.bfloat16)


def feed_forward(held, gate, up, down, other, ring_at):
    rows, wide = held[0].shape
    hidden = gate.shape[1]
    length = rows - 8

    def slots(owners):
        return [jnp.mod(ring_at + k, RING).astype(jnp.int32) for k in owners]

    def weight_specs():
        return [
            pl.BlockSpec((wide, hidden), lambda i, at: (at[0, i], 0)),
            pl.BlockSpec((wide, hidden), lambda i, at: (at[0, i], 0)),
            pl.BlockSpec((1, wide, 2 * hidden), lambda i, at: (at[0, i], 0, 0)),
        ]

    sums = [
        jax.ShapeDtypeStruct((length, 4 * hidden), jnp.float32),
        jax.ShapeDtypeStruct((8, length), jnp.float32),
    ]
    acc, squares = pl.pallas_call(
        gate_kernel,
        grid_spec=pltpu.PrefetchScalarGridSpec(
            num_scalar_prefetch=1,
            grid=(len(EARLY),),
            in_specs=[whole((rows, wide))] * len(EARLY) + weight_specs(),
            out_specs=[whole(s.shape) for s in sums],
            scratch_shapes=[pltpu.VMEM((rows, wide), jnp.bfloat16)],
        ),
        out_shape=sums,
        cost_estimate=pl.CostEstimate(
            flops=2 * length * wide * 4 * hidden * len(EARLY),
            bytes_accessed=5 * 10**6,
            transcendentals=0,
        ),
        name="gate_early",
    )(jnp.stack(slots(EARLY))[None], *[held[k] for k in EARLY], gate, up, other)

    late, send = slots(LATE), slots(SEND)
    table = jnp.stack(
        [jnp.stack(late + [late[-1]] * RING), jnp.stack([send[0]] * len(LATE) + send)]
    )
    grid = len(LATE) + RING
    return pl.pallas_call(
        functools.partial(down_kernel, float(wide * RING)),
        grid_spec=pltpu.PrefetchScalarGridSpec(
            num_scalar_prefetch=1,
            grid=(grid,),
            in_specs=[whole((rows, wide))] * len(LATE)
            + weight_specs()
            + [whole(s.shape) for s in sums]
            + [
                pl.BlockSpec((hidden, wide), lambda i, at: (0, at[1, i])),
                pl.BlockSpec((1, hidden, wide), lambda i, at: (at[1, i], 2 * hidden // hidden, 0)),
            ],
            out_specs=pl.BlockSpec(
                (1, length, wide), lambda i, at: (jnp.maximum(i - len(LATE), 0), 0, 0)
            ),
            scratch_shapes=[
                pltpu.VMEM((rows, wide), jnp.bfloat16),
                pltpu.VMEM((length, 4 * hidden), jnp.float32),
                pltpu.VMEM((8, length), jnp.float32),
                pltpu.VMEM((length, 2 * hidden), jnp.bfloat16),
            ],
        ),
        out_shape=jax.ShapeDtypeStruct((RING, length, wide), jnp.bfloat16),
        cost_estimate=pl.CostEstimate(
            flops=2 * length * wide * hidden * (4 * len(LATE) + 2 * RING),
            bytes_accessed=7 * 10**6,
            transcendentals=0,
        ),
        name="gate_late_and_down",
    )(table, *[held[k] for k in LATE], gate, up, other, acc, squares, down, other)


def spread(values, gain):
    rows, width = values.shape
    as_float = values.astype(jnp.float32)
    squares = jnp.sum(as_float * as_float, axis=1)
    gained = (as_float * gain.astype(jnp.float32)).astype(jnp.bfloat16)
    line = jnp.concatenate([squares, jnp.zeros((width - rows,), jnp.float32)])
    tail = jnp.broadcast_to(line.astype(jnp.bfloat16)[None], (8, width))
    return ring_gather(jnp.concatenate([gained, tail], axis=0))


def on_device(
    tokens,
    attn_gain,
    query_weight,
    key_weight,
    value_projection_matrix,
    attention_output_matrix,
    bucket_bias_matrix,
    ffn_gain,
    gate_weight,
    up_weight,
    down_projection_weight,
):
    sequences, length, part = tokens.shape
    half = lax.axis_index("row")
    ring_at = lax.axis_index("ma_0")
    copy_at = lax.axis_index("ba")
    copies = lax.axis_size("ba")
    token_rows = tokens.reshape(length, part)

    gains = jnp.concatenate(
        [attn_gain[None], ffn_gain[None], jnp.zeros((6, part), jnp.bfloat16)], axis=0
    )
    mine = jnp.concatenate([token_rows, gains], axis=0)
    theirs = lax.ppermute(mine, "ma_1", SWAP)

    half_rows = query_weight.shape[0]
    depth = half_rows // copies
    share = [
        lax.dynamic_slice_in_dim(w, copy_at * depth, depth, 0)
        for w in (query_weight, key_weight, value_projection_matrix)
    ]
    out_width = attention_output_matrix.shape[1] // copies
    share.append(
        lax.dynamic_slice_in_dim(attention_output_matrix, copy_at * out_width, out_width, 1)
    )
    first_share = lax.ppermute(jnp.concatenate(share, axis=1), "row", SWAP)
    other_first = lax.all_gather(first_share, "ba", axis=0, tiled=True)

    gate_depth = gate_weight.shape[0] // copies
    gate_share = [
        lax.dynamic_slice_in_dim(w, copy_at * gate_depth, gate_depth, 0)
        for w in (gate_weight, up_weight)
    ]
    down_width = down_projection_weight.shape[1] // copies
    down_share = lax.dynamic_slice_in_dim(
        down_projection_weight, copy_at * down_width, down_width, 1
    )
    second_share = jnp.concatenate([jnp.concatenate(gate_share, axis=1), down_share], axis=0)
    second_share = tied(second_share, theirs)
    second_share = lax.ppermute(second_share, "row", SWAP)
    second_share = tied(second_share, other_first)
    other_second = lax.all_gather(second_share, "ba", axis=0, tiled=False)

    wide = pair_order(mine, theirs, 1)
    wide_tokens = wide[:length]
    wide_attn_gain = wide[length]
    wide_ffn_gain = wide[length + 1]

    held = spread(wide_tokens, wide_attn_gain)
    out_blocks = attention(
        held,
        position_bias(bucket_bias_matrix, length),
        (query_weight, key_weight, value_projection_matrix),
        other_first,
        attention_output_matrix,
        ring_at,
        half,
    )
    summed = ring_sum(out_blocks).astype(jnp.bfloat16)
    partner = lax.ppermute(summed, "ma_1", SWAP)
    attn_out = summed.astype(jnp.float32) + partner.astype(jnp.float32)
    residual = (wide_tokens.astype(jnp.float32) + attn_out).astype(jnp.bfloat16)
    first = lax.axis_index("ma_1") == 0
    own_residual = jnp.where(first, residual[:, :part], residual[:, part:])

    held = spread(residual, wide_ffn_gain)
    summed = ring_sum(
        feed_forward(held, gate_weight, up_weight, down_projection_weight, other_second, ring_at)
    )
    low, high = summed[:, :part], summed[:, part:]
    keep = jnp.where(first, low, high)
    give = jnp.where(first, high, low).astype(jnp.bfloat16)
    got = lax.ppermute(give, "ma_1", SWAP)
    encoded = own_residual.astype(jnp.float32) + keep + got.astype(jnp.float32)
    return encoded.astype(jnp.bfloat16).reshape(sequences, length, part)


def solution(mesh):
    split = Mesh(
        mesh.devices.reshape(mesh.shape["ba"], RING, 2, mesh.shape["row"]),
        ("ba", "ma_0", "ma_1", "row"),
    )
    return jax.shard_map(
        on_device,
        mesh=split,
        in_specs=(
            P(("ba", "row"), None, MA),
            P(MA),
            P("row", MA),
            P("row", MA),
            P("row", MA),
            P(MA, "row"),
            P(None, MA),
            P(MA),
            P(None, MA_ROW),
            P(None, MA_ROW),
            P(MA_ROW, None),
        ),
        out_specs=P(("ba", "row"), None, MA),
        check_vma=False,
    )
```

```python
import functools

import jax
import jax.numpy as jnp
from jax import lax
from jax.experimental import pallas as pl
from jax.experimental.pallas import tpu as pltpu
from jax.sharding import Mesh
from jax.sharding import PartitionSpec as P

MA = ("ma_0", "ma_1")
MA_ROW = ("ma_0", "ma_1", "row")

bucket_thresholds = (1, 2, 3, 4, 5, 6, 7, 8, 11, 16, 23, 32, 45, 64, 91, 128)
epsilon = 1e-06
RING = 8
SWAP = [(0, 1), (1, 0)]
UP = [(i, (i + 1) % RING) for i in range(RING)]
DOWN = [(i, (i - 1) % RING) for i in range(RING)]


def tied(value, *after):
    return lax.optimization_barrier((value, *after))[0]


def pair_order(mine, theirs, axis):
    first = lax.axis_index("ma_1") == 0
    return jnp.where(
        first,
        jnp.concatenate([mine, theirs], axis=axis),
        jnp.concatenate([theirs, mine], axis=axis),
    )


def ring_gather(block):
    held = {0: block}
    above = below = block
    for step in range(1, RING // 2 + 1):
        above = lax.ppermute(above, "ma_0", DOWN)
        held[step] = above
        if step < RING // 2:
            below = lax.ppermute(below, "ma_0", UP)
            held[RING - step] = below
    return held


SEND = (4, 5, 3, 6, 2, 7, 1, 0)


def ring_sum(stack):
    def block(owner):
        return stack[SEND.index(owner % RING)].astype(jnp.float32)

    up, down = stack[0], stack[1]
    got_down = None
    for step in range(1, RING // 2 + 1):
        got_up = lax.ppermute(up, "ma_0", UP)
        if step > 1:
            got_down = lax.ppermute(down, "ma_0", DOWN)
        if step < RING // 2:
            up = (got_up.astype(jnp.float32) + block(4 - step)).astype(jnp.bfloat16)
            if got_down is not None:
                down = (got_down.astype(jnp.float32) + block(step - 4)).astype(jnp.bfloat16)
    return got_up.astype(jnp.float32) + got_down.astype(jnp.float32) + block(0)


def bias_kernel(bucket_ref, table_ref, bias_ref):
    heads, rows, columns = bias_ref.shape
    row = bucket_ref[0:1, :]
    for h in range(heads):
        line = jnp.zeros(row.shape, jnp.float32)
        for b in range(table_ref.shape[0]):
            line = jnp.where(row == b, table_ref[b : b + 1, h : h + 1], line)
        wide = jnp.broadcast_to(line, (rows, row.shape[1]))
        bias_ref[h] = pltpu.roll(wide, 0, 1, stride=1, stride_axis=0)[:, :columns]


def position_bias(table, length):
    offset = jnp.arange(2 * length, dtype=jnp.int32)
    offset = jnp.where(offset < length, offset, offset - 2 * length)
    distance = jnp.abs(offset)
    bucket = jnp.where(offset > 0, 15, 0)
    for threshold in bucket_thresholds[:15]:
        bucket = bucket + (distance >= threshold).astype(jnp.int32)
    last = (distance >= bucket_thresholds[15]) & (offset > 0)
    bucket = bucket + last.astype(jnp.int32)
    heads = table.shape[1]
    return pl.pallas_call(
        bias_kernel,
        out_shape=jax.ShapeDtypeStruct((heads, length, length), jnp.float32),
        cost_estimate=pl.CostEstimate(flops=10**8, bytes_accessed=10**6, transcendentals=0),
        name="position_bias",
    )(jnp.broadcast_to(bucket[None], (8, 2 * length)), table)


def as_column(line):
    size = line.shape[1]
    at_row = lax.broadcasted_iota(jnp.int32, (size, size), 0)
    at_column = lax.broadcasted_iota(jnp.int32, (size, size), 1)
    spread_out = jnp.where(at_row == at_column, jnp.broadcast_to(line, (size, size)), 0.0)
    return jnp.sum(spread_out, axis=1, keepdims=True)


def dot(a, b):
    return jnp.dot(a, b, preferred_element_type=jnp.float32)


def attention_kernel(width, at_ref, *refs):
    blocks = refs[:RING]
    own = refs[RING : RING + 3]
    other_ref, own_out_ref, other_out_ref, bias_ref = refs[RING + 3 : RING + 7]
    out_ref, x_ref, w_ref, o_ref, acc_ref, attended_ref = refs[RING + 7 : RING + 13]
    x_sem, own_sem, other_sem, o_sem = refs[RING + 13 :]
    length = acc_ref.shape[0]
    inner = attended_ref.shape[1]
    wide = x_ref.shape[2]
    parts = RING // 2
    rows = parts * wide

    own_copies = [
        pltpu.make_async_copy(
            own[k], w_ref.at[pl.ds(0, rows), pl.ds(k * inner, inner)], own_sem.at[k]
        )
        for k in range(3)
    ]
    x_copies = [
        pltpu.make_async_copy(blocks[k], x_ref.at[k], x_sem.at[k]) for k in range(RING)
    ]
    other_copies = [
        pltpu.make_async_copy(
            other_ref.at[pl.ds(k * wide, wide), :],
            w_ref.at[pl.ds(rows + k * wide, wide), :],
            other_sem.at[k],
        )
        for k in range(parts)
    ]
    o_copies = [
        pltpu.make_async_copy(ref, o_ref.at[k], o_sem.at[k])
        for k, ref in enumerate((own_out_ref, other_out_ref))
    ]
    for copy in x_copies + own_copies + other_copies + o_copies:
        copy.start()
    for copy in x_copies:
        copy.wait()
    squares = x_ref[0, length : length + 1, :length].astype(jnp.float32)
    for k in range(1, RING):
        squares += x_ref[k, length : length + 1, :length].astype(jnp.float32)
    scale = as_column(lax.rsqrt(squares / width + epsilon))
    for copy in own_copies:
        copy.wait()
    acc_ref[...] = jnp.zeros_like(acc_ref)

    def add_slot(slot, unused):
        weights = w_ref[pl.ds(pl.multiple_of(slot * wide, wide), wide), :]
        acc_ref[...] += dot(x_ref[at_ref[slot], :length, :], weights)
        return unused

    lax.fori_loop(0, parts, add_slot, 0)
    for copy in other_copies:
        copy.wait()
    lax.fori_loop(parts, RING, add_slot, 0)

    query, key, value = (
        (acc_ref[:, k * inner : (k + 1) * inner] * scale).astype(jnp.bfloat16) for k in range(3)
    )
    heads = bias_ref.shape[0]
    size = inner // heads
    for h in range(heads):
        at = slice(h * size, (h + 1) * size)
        scores = (
            lax.dot_general(
                query[:, at],
                key[:, at],
                (((1,), (1,)), ((), ())),
                preferred_element_type=jnp.float32,
            )
            + bias_ref[h]
        )
        exponent = jnp.exp(scores - jnp.max(scores, axis=-1, keepdims=True))
        weights = exponent / jnp.sum(exponent, axis=-1, keepdims=True)
        attended_ref[:, at] = dot(weights.astype(jnp.bfloat16), value[:, at]).astype(jnp.bfloat16)

    for copy in o_copies:
        copy.wait()

    def out_block(j, unused):
        slot = at_ref[RING + j]
        which = slot // parts
        column = pl.multiple_of((slot - which * parts) * wide, wide)
        out_ref[j] = dot(attended_ref[...], o_ref[which, :, pl.ds(column, wide)]).astype(
            jnp.bfloat16
        )
        return unused

    lax.fori_loop(0, RING, out_block, 0)


ANY = pl.BlockSpec(memory_space=pl.ANY)
SMEM = pl.BlockSpec(memory_space=pltpu.SMEM)
IN_VMEM = pl.BlockSpec(memory_space=pltpu.VMEM)


def attention(held, bias, own, other, own_out, other_out, ring_at, half):
    length = bias.shape[1]
    inner = own[0].shape[1]
    rows, wide = held[0].shape
    parts = RING // 2
    slot = jnp.arange(RING, dtype=jnp.int32)
    block_of = jnp.mod(slot + half * parts - ring_at, RING)
    slot_of = jnp.mod(jnp.asarray(SEND, jnp.int32) + ring_at + half * parts, RING)
    table = jnp.concatenate([block_of, slot_of]).astype(jnp.int32)
    return pl.pallas_call(
        functools.partial(attention_kernel, float(wide * RING)),
        in_specs=[SMEM] + [ANY] * (RING + 6) + [IN_VMEM],
        out_specs=IN_VMEM,
        scratch_shapes=[
            pltpu.VMEM((RING, rows, wide), jnp.bfloat16),
            pltpu.VMEM((RING * wide, 3 * inner), jnp.bfloat16),
            pltpu.VMEM((2, *own_out.shape), jnp.bfloat16),
            pltpu.VMEM((length, 3 * inner), jnp.float32),
            pltpu.VMEM((length, inner), jnp.bfloat16),
            pltpu.SemaphoreType.DMA((RING,)),
            pltpu.SemaphoreType.DMA((3,)),
            pltpu.SemaphoreType.DMA((parts,)),
            pltpu.SemaphoreType.DMA((2,)),
        ],
        out_shape=jax.ShapeDtypeStruct((RING, length, wide), jnp.bfloat16),
        cost_estimate=pl.CostEstimate(
            flops=2 * length * wide * RING * 4 * inner, bytes_accessed=10**7, transcendentals=0
        ),
        name="attention",
    )(
        table,
        *[held[k] for k in range(RING)],
        *own,
        other,
        own_out,
        other_out,
        bias,
    )


EARLY = (0, 1, 7, 2, 6)
LATE = (3, 5, 4)


def gate_copies(at_ref, blocks, gate_ref, up_ref, other_ref, x_ref, w_ref, x_sem, w_sem):
    wide, hidden = x_ref.shape[2], gate_ref.shape[1]
    copies = []
    for k, block in enumerate(blocks):
        row = pl.ds(pl.multiple_of(at_ref[k] * wide, wide), wide)
        copies.append(
            (
                pltpu.make_async_copy(block, x_ref.at[k], x_sem.at[k]),
                pltpu.make_async_copy(
                    gate_ref.at[row, :], w_ref.at[k, :, pl.ds(0, hidden)], w_sem.at[k, 0]
                ),
                pltpu.make_async_copy(
                    up_ref.at[row, :], w_ref.at[k, :, pl.ds(hidden, hidden)], w_sem.at[k, 1]
                ),
                pltpu.make_async_copy(
                    other_ref.at[at_ref[k], pl.ds(0, wide), :],
                    w_ref.at[k, :, pl.ds(2 * hidden, 2 * hidden)],
                    w_sem.at[k, 2],
                ),
            )
        )
    return copies


def start(copies):
    for group in copies:
        for copy in group:
            copy.start()


def gate_products(copies, x_ref, w_ref, acc_ref, squares_ref):
    length = acc_ref.shape[0]
    for group in copies:
        for copy in group:
            copy.wait()

    def add_block(k, unused):
        squares_ref[...] += x_ref[k, length : length + 8, :length].astype(jnp.float32)
        acc_ref[...] += dot(x_ref[k, :length, :], w_ref[k])
        return unused

    lax.fori_loop(0, len(copies), add_block, 0)


def gate_kernel(at_ref, *refs):
    count = len(EARLY)
    blocks = refs[:count]
    gate_ref, up_ref, other_ref, acc_ref, squares_ref, x_ref, w_ref, x_sem, w_sem = refs[count:]
    copies = gate_copies(at_ref, blocks, gate_ref, up_ref, other_ref, x_ref, w_ref, x_sem, w_sem)
    start(copies)
    acc_ref[...] = jnp.zeros_like(acc_ref)
    squares_ref[...] = jnp.zeros_like(squares_ref)
    gate_products(copies, x_ref, w_ref, acc_ref, squares_ref)


def down_kernel(width, at_ref, *refs):
    count = len(LATE)
    blocks = refs[:count]
    gate_ref, up_ref, other_ref, down_ref, acc_in_ref, squares_in_ref = refs[count : count + 6]
    out_ref, x_ref, w_ref, d_ref, acc_ref, squares_ref, hidden_ref = refs[count + 6 : count + 13]
    x_sem, w_sem, d_sem = refs[count + 13 :]
    size = gate_ref.shape[1]
    wide = x_ref.shape[2]
    copies = gate_copies(at_ref, blocks, gate_ref, up_ref, other_ref, x_ref, w_ref, x_sem, w_sem)
    start(copies)
    down_copies = []
    for j in range(RING):
        slot = at_ref[count + j]
        column = pl.ds(pl.multiple_of(slot * wide, wide), wide)
        down_copies.append(
            (
                pltpu.make_async_copy(
                    down_ref.at[:, column], d_ref.at[j, pl.ds(0, size), :], d_sem.at[j, 0]
                ),
                pltpu.make_async_copy(
                    other_ref.at[slot, pl.ds(wide, size), :],
                    d_ref.at[j, pl.ds(size, size), :],
                    d_sem.at[j, 1],
                ),
            )
        )
    start(down_copies)
    acc_ref[...] = acc_in_ref[...]
    squares_ref[...] = squares_in_ref[...]
    gate_products(copies, x_ref, w_ref, acc_ref, squares_ref)
    mean = squares_ref[0:1, :] / width
    scale = as_column(lax.rsqrt(mean + epsilon))
    for k in range(2):
        gate = acc_ref[:, 2 * k * size : (2 * k + 1) * size] * scale
        up = acc_ref[:, (2 * k + 1) * size : (2 * k + 2) * size] * scale
        hidden_ref[:, k * size : (k + 1) * size] = (
            jax.nn.gelu(gate, approximate=True) * up
        ).astype(jnp.bfloat16)
    for group in down_copies:
        for copy in group:
            copy.wait()

    def out_block(j, unused):
        out_ref[j] = dot(hidden_ref[...], d_ref[j]).astype(jnp.bfloat16)
        return unused

    lax.fori_loop(0, RING, out_block, 0)


def feed_forward(held, gate, up, down, other, ring_at):
    rows, wide = held[0].shape
    hidden = gate.shape[1]
    length = rows - 8

    def slots(owners):
        return jnp.mod(jnp.asarray(owners, jnp.int32) + ring_at, RING).astype(jnp.int32)

    def scratch(count):
        return [
            pltpu.VMEM((count, rows, wide), jnp.bfloat16),
            pltpu.VMEM((count, wide, 4 * hidden), jnp.bfloat16),
        ]

    sums = [
        jax.ShapeDtypeStruct((length, 4 * hidden), jnp.float32),
        jax.ShapeDtypeStruct((8, length), jnp.float32),
    ]
    early, late = len(EARLY), len(LATE)
    acc, squares = pl.pallas_call(
        gate_kernel,
        in_specs=[SMEM] + [ANY] * (early + 3),
        out_specs=[IN_VMEM] * 2,
        scratch_shapes=scratch(early)
        + [pltpu.SemaphoreType.DMA((early,)), pltpu.SemaphoreType.DMA((early, 3))],
        out_shape=sums,
        cost_estimate=pl.CostEstimate(
            flops=2 * length * wide * 4 * hidden * early,
            bytes_accessed=5 * 10**6,
            transcendentals=0,
        ),
        name="gate_early",
    )(slots(EARLY), *[held[k] for k in EARLY], gate, up, other)

    return pl.pallas_call(
        functools.partial(down_kernel, float(wide * RING)),
        in_specs=[SMEM] + [ANY] * (late + 4) + [IN_VMEM] * 2,
        out_specs=IN_VMEM,
        scratch_shapes=scratch(late)
        + [
            pltpu.VMEM((RING, 2 * hidden, wide), jnp.bfloat16),
            pltpu.VMEM((length, 4 * hidden), jnp.float32),
            pltpu.VMEM((8, length), jnp.float32),
            pltpu.VMEM((length, 2 * hidden), jnp.bfloat16),
            pltpu.SemaphoreType.DMA((late,)),
            pltpu.SemaphoreType.DMA((late, 3)),
            pltpu.SemaphoreType.DMA((RING, 2)),
        ],
        out_shape=jax.ShapeDtypeStruct((RING, length, wide), jnp.bfloat16),
        cost_estimate=pl.CostEstimate(
            flops=2 * length * wide * hidden * (4 * late + 2 * RING),
            bytes_accessed=7 * 10**6,
            transcendentals=0,
        ),
        name="gate_late_and_down",
    )(slots(LATE + SEND), *[held[k] for k in LATE], gate, up, other, down, acc, squares)


def spread(values, gain):
    rows, width = values.shape
    as_float = values.astype(jnp.float32)
    squares = jnp.sum(as_float * as_float, axis=1)
    gained = (as_float * gain.astype(jnp.float32)).astype(jnp.bfloat16)
    line = jnp.concatenate([squares, jnp.zeros((width - rows,), jnp.float32)])
    tail = jnp.broadcast_to(line.astype(jnp.bfloat16)[None], (8, width))
    return ring_gather(jnp.concatenate([gained, tail], axis=0))


def layer(
    tokens,
    attn_gain,
    query_weight,
    key_weight,
    value_projection_matrix,
    attention_output_matrix,
    bucket_bias_matrix,
    ffn_gain,
    gate_weight,
    up_weight,
    down_projection_weight,
):
    sequences, length, part = tokens.shape
    half = lax.axis_index("row")
    ring_at = lax.axis_index("ma_0")
    copy_at = lax.axis_index("ba")
    copies = lax.axis_size("ba")
    token_rows = tokens.reshape(length, part)

    gains = jnp.concatenate(
        [attn_gain[None], ffn_gain[None], jnp.zeros((6, part), jnp.bfloat16)], axis=0
    )
    mine = jnp.concatenate([token_rows, gains], axis=0)
    theirs = lax.ppermute(mine, "ma_1", SWAP)

    half_rows = query_weight.shape[0]
    depth = half_rows // copies
    share = [
        lax.dynamic_slice_in_dim(w, copy_at * depth, depth, 0)
        for w in (query_weight, key_weight, value_projection_matrix)
    ]
    first_share = lax.ppermute(jnp.concatenate(share, axis=1), "row", SWAP)
    other_first = lax.all_gather(first_share, "ba", axis=0, tiled=True)
    other_out = lax.ppermute(tied(attention_output_matrix, theirs), "row", SWAP)

    gate_depth = gate_weight.shape[0] // copies
    gate_share = [
        lax.dynamic_slice_in_dim(w, copy_at * gate_depth, gate_depth, 0)
        for w in (gate_weight, up_weight)
    ]
    down_width = down_projection_weight.shape[1] // copies
    down_share = lax.dynamic_slice_in_dim(
        down_projection_weight, copy_at * down_width, down_width, 1
    )
    second_share = jnp.concatenate([jnp.concatenate(gate_share, axis=1), down_share], axis=0)

    wide = pair_order(mine, theirs, 1)
    wide_tokens = wide[:length]
    wide_attn_gain = wide[length]
    wide_ffn_gain = wide[length + 1]

    held = spread(wide_tokens, wide_attn_gain)
    second_share = lax.ppermute(tied(second_share, held[1]), "row", SWAP)
    out_blocks = attention(
        held,
        position_bias(bucket_bias_matrix, length),
        (query_weight, key_weight, value_projection_matrix),
        other_first,
        attention_output_matrix,
        other_out,
        ring_at,
        half,
    )
    second_share = tied(second_share, out_blocks)
    other_second = lax.all_gather(second_share, "ba", axis=0, tiled=False)
    summed = ring_sum(out_blocks).astype(jnp.bfloat16)
    partner = lax.ppermute(summed, "ma_1", SWAP)
    attn_out = summed.astype(jnp.float32) + partner.astype(jnp.float32)
    residual = (wide_tokens.astype(jnp.float32) + attn_out).astype(jnp.bfloat16)
    first = lax.axis_index("ma_1") == 0
    own_residual = jnp.where(first, residual[:, :part], residual[:, part:])

    held = spread(residual, wide_ffn_gain)
    summed = ring_sum(
        feed_forward(held, gate_weight, up_weight, down_projection_weight, other_second, ring_at)
    )
    low, high = summed[:, :part], summed[:, part:]
    keep = jnp.where(first, low, high)
    give = jnp.where(first, high, low).astype(jnp.bfloat16)
    got = lax.ppermute(give, "ma_1", SWAP)
    encoded = own_residual.astype(jnp.float32) + keep + got.astype(jnp.float32)
    return encoded.astype(jnp.bfloat16).reshape(sequences, length, part)


def solution(mesh):
    split = Mesh(
        mesh.devices.reshape(mesh.shape["ba"], RING, 2, mesh.shape["row"]),
        ("ba", "ma_0", "ma_1", "row"),
    )
    return jax.shard_map(
        layer,
        mesh=split,
        in_specs=(
            P(("ba", "row"), None, MA),
            P(MA),
            P("row", MA),
            P("row", MA),
            P("row", MA),
            P(MA, "row"),
            P(None, MA),
            P(MA),
            P(None, MA_ROW),
            P(None, MA_ROW),
            P(MA_ROW, None),
        ),
        out_specs=P(("ba", "row"), None, MA),
        check_vma=False,
    )
```

```python
import functools

import jax
import jax.numpy as jnp
from jax import lax
from jax.experimental import pallas as pl
from jax.experimental.pallas import tpu as pltpu
from jax.sharding import Mesh
from jax.sharding import PartitionSpec as P

MA = ("ma_0", "ma_1")
MA_ROW = ("ma_0", "ma_1", "row")

bucket_thresholds = (1, 2, 3, 4, 5, 6, 7, 8, 11, 16, 23, 32, 45, 64, 91, 128)
epsilon = 1e-06
RING = 8
SWAP = [(0, 1), (1, 0)]
UP = [(i, (i + 1) % RING) for i in range(RING)]
DOWN = [(i, (i - 1) % RING) for i in range(RING)]


def tied(value, *after):
    return lax.optimization_barrier((value, *after))[0]


def pair_order(mine, theirs, axis):
    first = lax.axis_index("ma_1") == 0
    return jnp.where(
        first,
        jnp.concatenate([mine, theirs], axis=axis),
        jnp.concatenate([theirs, mine], axis=axis),
    )


def ring_gather(block):
    held = {0: block}
    above = below = block
    for step in range(1, RING // 2 + 1):
        above = lax.ppermute(above, "ma_0", DOWN)
        held[step] = above
        if step < RING // 2:
            below = lax.ppermute(below, "ma_0", UP)
            held[RING - step] = below
    return held


SEND = (4, 5, 0, 1, 2, 3, 6, 7)


def ring_sum(first, second, rest):
    blocks = [first, second, *(rest[k] for k in range(RING - 2))]

    def block(owner):
        return blocks[SEND.index(owner % RING)].astype(jnp.float32)

    up, down = blocks[0], blocks[1]
    got_down = None
    for step in range(1, RING // 2 + 1):
        got_up = lax.ppermute(up, "ma_0", UP)
        if step > 1:
            got_down = lax.ppermute(down, "ma_0", DOWN)
        if step < RING // 2:
            up = (got_up.astype(jnp.float32) + block(4 - step)).astype(jnp.bfloat16)
            if got_down is not None:
                down = (got_down.astype(jnp.float32) + block(step - 4)).astype(jnp.bfloat16)
    return got_up.astype(jnp.float32) + got_down.astype(jnp.float32) + block(0)


def bias_kernel(bucket_ref, table_ref, bias_ref):
    heads, rows, columns = bias_ref.shape
    bucket = bucket_ref[...]
    lines = jnp.zeros(bucket.shape, jnp.float32)
    for b in range(table_ref.shape[1]):
        lines = jnp.where(bucket == b, table_ref[:, b : b + 1], lines)
    for h in range(heads):
        wide = jnp.broadcast_to(lines[h : h + 1, :], (rows, bucket.shape[1]))
        bias_ref[h] = pltpu.roll(wide, 0, 1, stride=1, stride_axis=0)[:, :columns]


def position_bias(table, length):
    offset = jnp.arange(2 * length, dtype=jnp.int32)
    offset = jnp.where(offset < length, offset, offset - 2 * length)
    distance = jnp.abs(offset)
    bucket = jnp.where(offset > 0, 15, 0)
    for threshold in bucket_thresholds[:15]:
        bucket = bucket + (distance >= threshold).astype(jnp.int32)
    last = (distance >= bucket_thresholds[15]) & (offset > 0)
    bucket = bucket + last.astype(jnp.int32)
    heads = table.shape[1]
    return pl.pallas_call(
        bias_kernel,
        out_shape=jax.ShapeDtypeStruct((heads, length, length), jnp.float32),
        cost_estimate=pl.CostEstimate(flops=10**8, bytes_accessed=10**6, transcendentals=0),
        name="position_bias",
    )(jnp.broadcast_to(bucket[None], (heads, 2 * length)), table.T)


def as_column(line):
    size = line.shape[1]
    at_row = lax.broadcasted_iota(jnp.int32, (size, size), 0)
    at_column = lax.broadcasted_iota(jnp.int32, (size, size), 1)
    spread_out = jnp.where(at_row == at_column, jnp.broadcast_to(line, (size, size)), 0.0)
    return jnp.sum(spread_out, axis=1, keepdims=True)


def dot(a, b):
    return jnp.dot(a, b, preferred_element_type=jnp.float32)


def attention_kernel(width, *refs):
    ring_at, half = lax.axis_index("ma_0"), lax.axis_index("row")
    blocks = refs[:RING]
    own = refs[RING : RING + 3]
    other_ref, own_out_ref, other_out_ref, bias_ref = refs[RING + 3 : RING + 7]
    out_refs = refs[RING + 7 : RING + 10]
    x_ref, w_ref, o_ref, acc_ref, attended_ref, both_ref = refs[RING + 10 : RING + 16]
    x_sem, own_sem, other_sem, o_sem = refs[RING + 16 :]
    length = acc_ref.shape[0]
    inner = attended_ref.shape[1]
    wide = x_ref.shape[2]
    parts = RING // 2
    rows = parts * wide

    own_copies = [
        pltpu.make_async_copy(
            own[k], w_ref.at[pl.ds(0, rows), pl.ds(k * inner, inner)], own_sem.at[k]
        )
        for k in range(3)
    ]
    x_copies = [
        pltpu.make_async_copy(blocks[k], x_ref.at[k], x_sem.at[k]) for k in range(RING)
    ]
    other_copies = [
        pltpu.make_async_copy(
            other_ref.at[pl.ds(k * wide, wide), :],
            w_ref.at[pl.ds(rows + k * wide, wide), :],
            other_sem.at[k],
        )
        for k in range(parts)
    ]
    o_copies = [
        pltpu.make_async_copy(ref, o_ref.at[k], o_sem.at[k])
        for k, ref in enumerate((own_out_ref, other_out_ref))
    ]
    for copy in x_copies + own_copies + other_copies + o_copies:
        copy.start()
    for copy in x_copies:
        copy.wait()
    squares = x_ref[0, length : length + 1, :length].astype(jnp.float32)
    for k in range(1, RING):
        squares += x_ref[k, length : length + 1, :length].astype(jnp.float32)
    scale = as_column(lax.rsqrt(squares / width + epsilon))
    for copy in own_copies:
        copy.wait()
    acc_ref[...] = jnp.zeros_like(acc_ref)

    def add_slot(slot, unused):
        weights = w_ref[pl.ds(pl.multiple_of(slot * wide, wide), wide), :]
        block = lax.rem(slot + half * parts + RING - ring_at, RING)
        acc_ref[...] += dot(x_ref[block, :length, :], weights)
        return unused

    lax.fori_loop(0, parts, add_slot, 0)
    for copy in other_copies:
        copy.wait()
    lax.fori_loop(parts, RING, add_slot, 0)

    heads = bias_ref.shape[0]
    size = inner // heads
    pair = 2 * size

    def two_heads(n, unused):
        query, key, value = (
            (acc_ref[:, pl.ds(pl.multiple_of(k * inner + n * pair, pair), pair)] * scale).astype(
                jnp.bfloat16
            )
            for k in range(3)
        )
        for h in range(2):
            at = slice(h * size, (h + 1) * size)
            scores = (
                lax.dot_general(
                    query[:, at],
                    key[:, at],
                    (((1,), (1,)), ((), ())),
                    preferred_element_type=jnp.float32,
                )
                + bias_ref[2 * n + h]
            )
            exponent = jnp.exp(scores - jnp.max(scores, axis=-1, keepdims=True))
            weights = exponent / jnp.sum(exponent, axis=-1, keepdims=True)
            both_ref[:, at] = dot(weights.astype(jnp.bfloat16), value[:, at]).astype(jnp.bfloat16)
        attended_ref[:, pl.ds(pl.multiple_of(n * pair, pair), pair)] = both_ref[...]
        return unused

    lax.fori_loop(0, heads // 2, two_heads, 0)

    for copy in o_copies:
        copy.wait()

    def out_block(owner):
        slot = lax.rem(ring_at + owner + half * parts, RING)
        which = slot // parts
        column = pl.multiple_of((slot - which * parts) * wide, wide)
        product = dot(attended_ref[...], o_ref[which, :, pl.ds(column, wide)])
        return product.astype(jnp.bfloat16)

    store_blocks(out_block, out_refs)


def store_blocks(block, out_refs):
    first_ref, second_ref, rest_ref = out_refs
    first_ref[...] = block(SEND[0])
    second_ref[...] = block(SEND[1])

    def store(k, unused):
        rest_ref[k] = block(jnp.where(k < 4, k, k + 2))
        return unused

    lax.fori_loop(0, RING - 2, store, 0)


def block_shapes(length, width):
    one = jax.ShapeDtypeStruct((length, width), jnp.bfloat16)
    return [one, one, jax.ShapeDtypeStruct((RING - 2, length, width), jnp.bfloat16)]


ANY = pl.BlockSpec(memory_space=pl.ANY)
IN_VMEM = pl.BlockSpec(memory_space=pltpu.VMEM)


def attention(held, bias, own, other, own_out, other_out):
    length = bias.shape[1]
    inner = own[0].shape[1]
    rows, wide = held[0].shape
    parts = RING // 2
    return pl.pallas_call(
        functools.partial(attention_kernel, float(wide * RING)),
        in_specs=[ANY] * (RING + 6) + [IN_VMEM],
        out_specs=[IN_VMEM] * 3,
        scratch_shapes=[
            pltpu.VMEM((RING, rows, wide), jnp.bfloat16),
            pltpu.VMEM((RING * wide, 3 * inner), jnp.bfloat16),
            pltpu.VMEM((2, *own_out.shape), jnp.bfloat16),
            pltpu.VMEM((length, 3 * inner), jnp.float32),
            pltpu.VMEM((length, inner), jnp.bfloat16),
            pltpu.VMEM((length, 2 * inner // bias.shape[0]), jnp.bfloat16),
            pltpu.SemaphoreType.DMA((RING,)),
            pltpu.SemaphoreType.DMA((3,)),
            pltpu.SemaphoreType.DMA((parts,)),
            pltpu.SemaphoreType.DMA((2,)),
        ],
        out_shape=block_shapes(length, wide),
        cost_estimate=pl.CostEstimate(
            flops=2 * length * wide * RING * 4 * inner, bytes_accessed=10**7, transcendentals=0
        ),
        name="attention",
    )(
        *[held[k] for k in range(RING)],
        *own,
        other,
        own_out,
        other_out,
        bias,
    )


FIRST = (0, 1, 7)
SECOND = (2, 6, 3, 5)
LAST = (4,)


def gate_copies(owners, blocks, gate_ref, up_ref, other_ref, x_ref, w_ref, x_sem, w_sem):
    wide, hidden = x_ref.shape[2], gate_ref.shape[1]
    ring_at = lax.axis_index("ma_0")
    copies = []
    for k, (owner, block) in enumerate(zip(owners, blocks)):
        slot = lax.rem(ring_at + owner, RING)
        row = pl.ds(pl.multiple_of(slot * wide, wide), wide)
        copies.append(pltpu.make_async_copy(block, x_ref.at[k], x_sem.at[k]))
        sources = [
            gate_ref.at[row, :],
            up_ref.at[row, :],
            other_ref.at[slot, pl.ds(0, wide), :],
            other_ref.at[slot, pl.ds(wide, wide), :],
        ]
        for n, source in enumerate(sources):
            copies.append(
                pltpu.make_async_copy(
                    source, w_ref.at[k, :, pl.ds(n * hidden, hidden)], w_sem.at[k, n]
                )
            )
    return copies


def gate_kernel(owners, more, *refs):
    count = len(owners)
    blocks = refs[:count]
    gate_ref, up_ref, other_ref = refs[count : count + 3]
    refs = refs[count + 3 :]
    if more:
        acc_in_ref, squares_in_ref, refs = refs[0], refs[1], refs[2:]
    acc_ref, squares_ref, x_ref, w_ref, x_sem, w_sem = refs
    length = acc_ref.shape[0]
    copies = gate_copies(owners, blocks, gate_ref, up_ref, other_ref, x_ref, w_ref, x_sem, w_sem)
    for copy in copies:
        copy.start()
    if more:
        acc_ref[...] = acc_in_ref[...]
        squares_ref[...] = squares_in_ref[...]
    else:
        acc_ref[...] = jnp.zeros_like(acc_ref)
        squares_ref[...] = jnp.zeros_like(squares_ref)
    for copy in copies:
        copy.wait()

    def add_block(k, unused):
        squares_ref[...] += x_ref[k, length : length + 8, :length].astype(jnp.float32)
        acc_ref[...] += dot(x_ref[k, :length, :], w_ref[k])
        return unused

    lax.fori_loop(0, count, add_block, 0)


def hidden_kernel(width, *refs):
    count = len(LAST)
    blocks = refs[:count]
    gate_ref, up_ref, other_ref, acc_in_ref, squares_in_ref = refs[count : count + 5]
    hidden_ref, x_ref, w_ref, x_sem, w_sem = refs[count + 5 :]
    size = gate_ref.shape[1]
    length = hidden_ref.shape[0]
    copies = gate_copies(LAST, blocks, gate_ref, up_ref, other_ref, x_ref, w_ref, x_sem, w_sem)
    for copy in copies:
        copy.start()
    for copy in copies:
        copy.wait()
    rows = x_ref[0, :length, :]
    squares = squares_in_ref[0:1, :] + x_ref[0, length : length + 1, :length].astype(jnp.float32)
    scale = as_column(lax.rsqrt(squares / width + epsilon))
    for k in range(2):
        sums = []
        for n in (2 * k, 2 * k + 1):
            at = slice(n * size, (n + 1) * size)
            sums.append((acc_in_ref[:, at] + dot(rows, w_ref[0, :, at])) * scale)
        hidden_ref[:, k * size : (k + 1) * size] = (
            jax.nn.gelu(sums[0], approximate=True) * sums[1]
        ).astype(jnp.bfloat16)


def down_copies(first_refs, d_ref, d_sem):
    copies = []
    ring_at = lax.axis_index("ma_0")
    for j in range(RING):
        slot = lax.rem(ring_at + j, RING)
        for n, source in enumerate(first_refs(slot)):
            rows = source.shape[0]
            copies.append(
                pltpu.make_async_copy(source, d_ref.at[j, pl.ds(n * rows, rows), :], d_sem.at[j, n])
            )
    return copies


def own_down_kernel(hidden_ref, down_ref, other_ref, out_ref, d_ref, d_sem):
    size = d_ref.shape[1] // 2
    part = d_ref.shape[2]
    pair_at = lax.axis_index("ma_1")

    def sources(slot):
        column = pl.multiple_of((slot * 2 + pair_at) * part, part)
        return down_ref.at[:, pl.ds(column, part)], other_ref.at[slot, pl.ds(4 * size, size), :]

    copies = down_copies(sources, d_ref, d_sem)
    for copy in copies:
        copy.start()
    for copy in copies:
        copy.wait()

    def block(j, unused):
        out_ref[j] = dot(hidden_ref[...], d_ref[j])
        return unused

    lax.fori_loop(0, RING, block, 0)


def pair_down_kernel(hidden_ref, other_ref, own_ref, *refs):
    out_refs, (d_ref, own_in_ref, d_sem, own_sem) = refs[:3], refs[3:]
    size = d_ref.shape[1] // 2
    own_copy = pltpu.make_async_copy(own_ref, own_in_ref, own_sem)
    own_copy.start()

    def sources(slot):
        return [other_ref.at[slot, pl.ds((5 + n) * size, size), :] for n in range(2)]

    copies = down_copies(sources, d_ref, d_sem)
    for copy in copies:
        copy.start()
    own_copy.wait()
    for copy in copies:
        copy.wait()

    def block(owner):
        return (own_in_ref[owner] + dot(hidden_ref[...], d_ref[owner])).astype(jnp.bfloat16)

    store_blocks(block, out_refs)


def feed_forward(held, gate, up, down, other):
    rows, wide = held[0].shape
    hidden = gate.shape[1]
    length = rows - 8
    part = wide // 2
    sums = [
        jax.ShapeDtypeStruct((length, 4 * hidden), jnp.float32),
        jax.ShapeDtypeStruct((8, length), jnp.float32),
    ]

    def scratch(count):
        return [
            pltpu.VMEM((count, rows, wide), jnp.bfloat16),
            pltpu.VMEM((count, wide, 4 * hidden), jnp.bfloat16),
            pltpu.SemaphoreType.DMA((count,)),
            pltpu.SemaphoreType.DMA((count, 4)),
        ]

    def cost(count, extra=0):
        return pl.CostEstimate(
            flops=2 * length * wide * 4 * hidden * count + extra,
            bytes_accessed=10**6 * (count + 1),
            transcendentals=0,
        )

    def gate_sums(owners, before):
        return pl.pallas_call(
            functools.partial(gate_kernel, owners, bool(before)),
            in_specs=[ANY] * (len(owners) + 3) + [IN_VMEM] * len(before),
            out_specs=[IN_VMEM] * 2,
            scratch_shapes=scratch(len(owners)),
            out_shape=sums,
            cost_estimate=cost(len(owners)),
        )(*[held[k] for k in owners], gate, up, other, *before)

    before = gate_sums(FIRST, ())
    before = gate_sums(SECOND, before)
    mine = pl.pallas_call(
        functools.partial(hidden_kernel, float(wide * RING)),
        in_specs=[ANY] * (len(LAST) + 3) + [IN_VMEM] * 2,
        out_specs=IN_VMEM,
        scratch_shapes=scratch(len(LAST)),
        out_shape=jax.ShapeDtypeStruct((length, 2 * hidden), jnp.bfloat16),
        cost_estimate=cost(1),
        name="hidden",
    )(*[held[k] for k in LAST], gate, up, other, *before)
    theirs = lax.ppermute(mine, "ma_1", SWAP)
    weights = [
        pltpu.VMEM((RING, 2 * hidden, part), jnp.bfloat16),
        pltpu.SemaphoreType.DMA((RING, 2)),
    ]
    own = pl.pallas_call(
        own_down_kernel,
        in_specs=[IN_VMEM, ANY, ANY],
        out_specs=IN_VMEM,
        scratch_shapes=weights,
        out_shape=jax.ShapeDtypeStruct((RING, length, part), jnp.float32),
        cost_estimate=cost(2),
        name="own_down",
    )(mine, down, other)
    return pl.pallas_call(
        pair_down_kernel,
        in_specs=[IN_VMEM, ANY, ANY],
        out_specs=[IN_VMEM] * 3,
        scratch_shapes=[
            weights[0],
            pltpu.VMEM((RING, length, part), jnp.float32),
            weights[1],
            pltpu.SemaphoreType.DMA,
        ],
        out_shape=block_shapes(length, part),
        cost_estimate=cost(2),
        name="pair_down",
    )(theirs, other, own)


def spread(values, gain):
    rows, width = values.shape
    as_float = values.astype(jnp.float32)
    squares = jnp.sum(as_float * as_float, axis=1)
    gained = (as_float * gain.astype(jnp.float32)).astype(jnp.bfloat16)
    line = jnp.concatenate([squares, jnp.zeros((width - rows,), jnp.float32)])
    tail = jnp.broadcast_to(line.astype(jnp.bfloat16)[None], (8, width))
    block = jnp.concatenate([gained, tail], axis=0)
    return ring_gather(block)


def layer(
    tokens,
    attn_gain,
    query_weight,
    key_weight,
    value_projection_matrix,
    attention_output_matrix,
    bucket_bias_matrix,
    ffn_gain,
    gate_weight,
    up_weight,
    down_projection_weight,
):
    sequences, length, part = tokens.shape
    copy_at = lax.axis_index("ba")
    copies = lax.axis_size("ba")
    token_rows = tokens.reshape(length, part)

    gains = jnp.concatenate(
        [attn_gain[None], ffn_gain[None], jnp.zeros((6, part), jnp.bfloat16)], axis=0
    )
    mine = jnp.concatenate([token_rows, gains], axis=0)
    theirs = lax.ppermute(mine, "ma_1", SWAP)

    half_rows = query_weight.shape[0]
    depth = half_rows // copies
    share = [
        lax.dynamic_slice_in_dim(w, copy_at * depth, depth, 0)
        for w in (query_weight, key_weight, value_projection_matrix)
    ]
    first_share = lax.ppermute(jnp.concatenate(share, axis=1), "row", SWAP)
    other_first = lax.all_gather(first_share, "ba", axis=0, tiled=True)
    other_out = lax.ppermute(tied(attention_output_matrix, theirs), "row", SWAP)

    gate_depth = gate_weight.shape[0] // copies
    gate_share = [
        lax.dynamic_slice_in_dim(w, copy_at * gate_depth, gate_depth, 0)
        for w in (gate_weight, up_weight)
    ]
    down_width = down_projection_weight.shape[1] // copies
    pair_at = lax.axis_index("ma_1")

    def down_share(pair):
        at = copy_at * down_width + pair * part
        return lax.dynamic_slice_in_dim(down_projection_weight, at, part, 1)

    row_share = jnp.concatenate([*gate_share, down_share(pair_at)], axis=0)
    pair_share = down_share(1 - pair_at)

    wide = pair_order(mine, theirs, 1)
    wide_tokens = wide[:length]
    wide_attn_gain = wide[length]
    wide_ffn_gain = wide[length + 1]

    held = spread(wide_tokens, wide_attn_gain)
    row_share = lax.ppermute(tied(row_share, held[1]), "row", SWAP)
    pair_share = tied(pair_share, held[2])
    cross = [(0, 3), (3, 0), (1, 2), (2, 1)]
    cross_share = lax.ppermute(pair_share, ("ma_1", "row"), cross)
    pair_share = lax.ppermute(pair_share, "ma_1", SWAP)
    out_blocks = attention(
        held,
        position_bias(bucket_bias_matrix, length),
        (query_weight, key_weight, value_projection_matrix),
        other_first,
        attention_output_matrix,
        other_out,
    )
    second_share = jnp.concatenate([row_share, pair_share, cross_share], axis=0)
    second_share = tied(second_share, out_blocks[0])
    other_second = lax.all_gather(second_share, "ba", axis=0, tiled=False)
    summed = ring_sum(*out_blocks).astype(jnp.bfloat16)
    partner = lax.ppermute(summed, "ma_1", SWAP)
    attn_out = summed.astype(jnp.float32) + partner.astype(jnp.float32)
    residual = (wide_tokens.astype(jnp.float32) + attn_out).astype(jnp.bfloat16)
    first = lax.axis_index("ma_1") == 0
    own_residual = jnp.where(first, residual[:, :part], residual[:, part:])

    held = spread(residual, wide_ffn_gain)
    summed = ring_sum(
        *feed_forward(held, gate_weight, up_weight, down_projection_weight, other_second)
    )
    encoded = own_residual.astype(jnp.float32) + summed
    return encoded.astype(jnp.bfloat16).reshape(sequences, length, part)


def solution(mesh):
    split = Mesh(
        mesh.devices.reshape(mesh.shape["ba"], RING, 2, mesh.shape["row"]),
        ("ba", "ma_0", "ma_1", "row"),
    )
    return jax.shard_map(
        layer,
        mesh=split,
        in_specs=(
            P(("ba", "row"), None, MA),
            P(MA),
            P("row", MA),
            P("row", MA),
            P("row", MA),
            P(MA, "row"),
            P(None, MA),
            P(MA),
            P(None, MA_ROW),
            P(None, MA_ROW),
            P(MA_ROW, None),
        ),
        out_specs=P(("ba", "row"), None, MA),
        check_vma=False,
    )
```

```python
import functools

import jax
import jax.numpy as jnp
from jax import lax
from jax.experimental import pallas as pl
from jax.experimental.pallas import tpu as pltpu
from jax.sharding import Mesh
from jax.sharding import PartitionSpec as P

MA = ("ma_0", "ma_1")
MA_ROW = ("ma_0", "ma_1", "row")

bucket_thresholds = (1, 2, 3, 4, 5, 6, 7, 8, 11, 16, 23, 32, 45, 64, 91, 128)
epsilon = 1e-06
RING = 8
SWAP = [(0, 1), (1, 0)]
UP = [(i, (i + 1) % RING) for i in range(RING)]
DOWN = [(i, (i - 1) % RING) for i in range(RING)]


def tied(value, *after):
    return lax.optimization_barrier((value, *after))[0]


def pair_order(mine, theirs, axis):
    first = lax.axis_index("ma_1") == 0
    return jnp.where(
        first,
        jnp.concatenate([mine, theirs], axis=axis),
        jnp.concatenate([theirs, mine], axis=axis),
    )


def ring_gather(block):
    held = {0: block}
    above = below = block
    for step in range(1, RING // 2 + 1):
        above = lax.ppermute(above, "ma_0", DOWN)
        held[step] = above
        if step < RING // 2:
            below = lax.ppermute(below, "ma_0", UP)
            held[RING - step] = below
    return held


SEND = (4, 5, 0, 1, 2, 3, 6, 7)


def ring_sum(first, second, rest):
    blocks = [first, second, *(rest[k] for k in range(RING - 2))]

    def block(owner):
        return blocks[SEND.index(owner % RING)].astype(jnp.float32)

    up, down = blocks[0], blocks[1]
    got_down = None
    for step in range(1, RING // 2 + 1):
        got_up = lax.ppermute(up, "ma_0", UP)
        if step > 1:
            got_down = lax.ppermute(down, "ma_0", DOWN)
        if step < RING // 2:
            up = (got_up.astype(jnp.float32) + block(4 - step)).astype(jnp.bfloat16)
            if got_down is not None:
                down = (got_down.astype(jnp.float32) + block(step - 4)).astype(jnp.bfloat16)
    return got_up.astype(jnp.float32) + got_down.astype(jnp.float32) + block(0)


def bias_kernel(bucket_ref, table_ref, bias_ref):
    heads, rows, columns = bias_ref.shape
    bucket = bucket_ref[...]
    lines = jnp.zeros(bucket.shape, jnp.float32)
    for b in range(table_ref.shape[1]):
        lines = jnp.where(bucket == b, table_ref[:, b : b + 1], lines)
    for h in range(heads):
        wide = jnp.broadcast_to(lines[h : h + 1, :], (rows, bucket.shape[1]))
        bias_ref[h] = pltpu.roll(wide, 0, 1, stride=1, stride_axis=0)[:, :columns]


def position_bias(table, length):
    offset = jnp.arange(2 * length, dtype=jnp.int32)
    offset = jnp.where(offset < length, offset, offset - 2 * length)
    distance = jnp.abs(offset)
    bucket = jnp.where(offset > 0, 15, 0)
    for threshold in bucket_thresholds[:15]:
        bucket = bucket + (distance >= threshold).astype(jnp.int32)
    last = (distance >= bucket_thresholds[15]) & (offset > 0)
    bucket = bucket + last.astype(jnp.int32)
    heads = table.shape[1]
    return pl.pallas_call(
        bias_kernel,
        out_shape=jax.ShapeDtypeStruct((heads, length, length), jnp.float32),
        cost_estimate=pl.CostEstimate(flops=10**8, bytes_accessed=10**6, transcendentals=0),
        name="position_bias",
    )(jnp.broadcast_to(bucket[None], (heads, 2 * length)), table.T)


def as_column(line):
    size = line.shape[1]
    at_row = lax.broadcasted_iota(jnp.int32, (size, size), 0)
    at_column = lax.broadcasted_iota(jnp.int32, (size, size), 1)
    spread_out = jnp.where(at_row == at_column, jnp.broadcast_to(line, (size, size)), 0.0)
    return jnp.sum(spread_out, axis=1, keepdims=True)


def dot(a, b):
    return jnp.dot(a, b, preferred_element_type=jnp.float32)


def attention_kernel(width, *refs):
    ring_at, half = lax.axis_index("ma_0"), lax.axis_index("row")
    blocks = refs[:RING]
    own = refs[RING : RING + 3]
    other_ref, *out_weight_refs, bias_ref = refs[RING + 3 : RING + 8]
    first_ref, second_ref, attended_ref = refs[RING + 8 : RING + 11]
    x_ref, w_ref, o_ref, acc_ref, both_ref = refs[RING + 11 : RING + 16]
    x_sem, own_sem, other_sem, o_sem = refs[RING + 16 :]
    length = acc_ref.shape[0]
    inner = attended_ref.shape[1]
    wide = x_ref.shape[2]
    parts = RING // 2
    rows = parts * wide

    own_copies = [
        pltpu.make_async_copy(
            own[k], w_ref.at[pl.ds(0, rows), pl.ds(k * inner, inner)], own_sem.at[k]
        )
        for k in range(3)
    ]
    x_copies = [
        pltpu.make_async_copy(blocks[k], x_ref.at[k], x_sem.at[k]) for k in range(RING)
    ]
    other_copies = [
        pltpu.make_async_copy(
            other_ref.at[pl.ds(k * wide, wide), :],
            w_ref.at[pl.ds(rows + k * wide, wide), :],
            other_sem.at[k],
        )
        for k in range(parts)
    ]
    o_copies = out_weight_copies(out_weight_refs, o_ref, o_sem)
    for copy in x_copies + own_copies + other_copies + o_copies:
        copy.start()
    for copy in x_copies:
        copy.wait()
    squares = x_ref[0, length : length + 1, :length].astype(jnp.float32)
    for k in range(1, RING):
        squares += x_ref[k, length : length + 1, :length].astype(jnp.float32)
    scale = as_column(lax.rsqrt(squares / width + epsilon))
    for copy in own_copies:
        copy.wait()
    acc_ref[...] = jnp.zeros_like(acc_ref)

    def add_slot(slot, unused):
        weights = w_ref[pl.ds(pl.multiple_of(slot * wide, wide), wide), :]
        block = lax.rem(slot + half * parts + RING - ring_at, RING)
        acc_ref[...] += dot(x_ref[block, :length, :], weights)
        return unused

    lax.fori_loop(0, parts, add_slot, 0)
    for copy in other_copies:
        copy.wait()
    lax.fori_loop(parts, RING, add_slot, 0)

    heads = bias_ref.shape[0]
    size = inner // heads
    pair = 2 * size

    def two_heads(n, unused):
        query, key, value = (
            (acc_ref[:, pl.ds(pl.multiple_of(k * inner + n * pair, pair), pair)] * scale).astype(
                jnp.bfloat16
            )
            for k in range(3)
        )
        for h in range(2):
            at = slice(h * size, (h + 1) * size)
            scores = (
                lax.dot_general(
                    query[:, at],
                    key[:, at],
                    (((1,), (1,)), ((), ())),
                    preferred_element_type=jnp.float32,
                )
                + bias_ref[2 * n + h]
            )
            exponent = jnp.exp(scores - jnp.max(scores, axis=-1, keepdims=True))
            weights = exponent / jnp.sum(exponent, axis=-1, keepdims=True)
            both_ref[:, at] = dot(weights.astype(jnp.bfloat16), value[:, at]).astype(jnp.bfloat16)
        attended_ref[:, pl.ds(pl.multiple_of(n * pair, pair), pair)] = both_ref[...]
        return unused

    lax.fori_loop(0, heads // 2, two_heads, 0)

    for copy in o_copies:
        copy.wait()

    first_ref[...] = out_block(SEND[0], attended_ref, o_ref)
    second_ref[...] = out_block(SEND[1], attended_ref, o_ref)


def out_weight_copies(refs, o_ref, o_sem):
    width = refs[1].shape[1]
    core = lax.rem(lax.axis_index("ba"), 2)
    targets = [
        o_ref.at[0],
        o_ref.at[1, :, pl.ds(pl.multiple_of(core * width, width), width)],
        o_ref.at[1, :, pl.ds(pl.multiple_of((1 - core) * width, width), width)],
    ]
    return [
        pltpu.make_async_copy(ref, target, o_sem.at[k])
        for k, (ref, target) in enumerate(zip(refs, targets))
    ]


def out_block(owner, attended_ref, o_ref):
    ring_at, half = lax.axis_index("ma_0"), lax.axis_index("row")
    parts = RING // 2
    wide = o_ref.shape[2] // parts
    slot = lax.rem(ring_at + owner + half * parts, RING)
    which = slot // parts
    column = pl.multiple_of((slot - which * parts) * wide, wide)
    product = dot(attended_ref[...], o_ref[which, :, pl.ds(column, wide)])
    return product.astype(jnp.bfloat16)


def out_rest_kernel(*refs):
    out_weight_refs = refs[1:4]
    attended_ref, rest_ref, o_ref, o_sem = refs[0], *refs[4:]
    copies = out_weight_copies(out_weight_refs, o_ref, o_sem)
    for copy in copies:
        copy.start()
    for copy in copies:
        copy.wait()
    store_rest(lambda owner: out_block(owner, attended_ref, o_ref), rest_ref)


def store_rest(block, rest_ref):
    def store(k, unused):
        rest_ref[k] = block(jnp.where(k < 4, k, k + 2))
        return unused

    lax.fori_loop(0, RING - 2, store, 0)


def one_block(length, width):
    return jax.ShapeDtypeStruct((length, width), jnp.bfloat16)


def rest_blocks(length, width):
    return jax.ShapeDtypeStruct((RING - 2, length, width), jnp.bfloat16)


ANY = pl.BlockSpec(memory_space=pl.ANY)
IN_VMEM = pl.BlockSpec(memory_space=pltpu.VMEM)


def attention(held, bias, own, other, out_weights):
    length = bias.shape[1]
    inner = own[0].shape[1]
    rows, wide = held[0].shape
    parts = RING // 2
    out_scratch = [
        pltpu.VMEM((2, *out_weights[0].shape), jnp.bfloat16),
        pltpu.SemaphoreType.DMA((3,)),
    ]
    first, second, attended = pl.pallas_call(
        functools.partial(attention_kernel, float(wide * RING)),
        in_specs=[ANY] * (RING + 7) + [IN_VMEM],
        out_specs=[IN_VMEM] * 3,
        scratch_shapes=[
            pltpu.VMEM((RING, rows, wide), jnp.bfloat16),
            pltpu.VMEM((RING * wide, 3 * inner), jnp.bfloat16),
            out_scratch[0],
            pltpu.VMEM((length, 3 * inner), jnp.float32),
            pltpu.VMEM((length, 2 * inner // bias.shape[0]), jnp.bfloat16),
            pltpu.SemaphoreType.DMA((RING,)),
            pltpu.SemaphoreType.DMA((3,)),
            pltpu.SemaphoreType.DMA((parts,)),
            out_scratch[1],
        ],
        out_shape=[one_block(length, wide)] * 2 + [one_block(length, inner)],
        cost_estimate=pl.CostEstimate(
            flops=2 * length * wide * RING * 4 * inner, bytes_accessed=10**7, transcendentals=0
        ),
        name="attention",
    )(
        *[held[k] for k in range(RING)],
        *own,
        other,
        *out_weights,
        bias,
    )
    rest = pl.pallas_call(
        out_rest_kernel,
        in_specs=[IN_VMEM] + [ANY] * 3,
        out_specs=IN_VMEM,
        scratch_shapes=out_scratch,
        out_shape=rest_blocks(length, wide),
        cost_estimate=pl.CostEstimate(
            flops=2 * length * inner * wide * (RING - 2),
            bytes_accessed=4 * 10**6,
            transcendentals=0,
        ),
        name="out_rest",
    )(attended, *out_weights)
    return first, second, rest


FIRST = (0, 1, 7)
SECOND = (2, 6)
THIRD = (3, 5)
LAST = (4,)


def gate_copies(owners, blocks, gate_ref, up_ref, other_ref, x_ref, w_ref, x_sem, w_sem):
    wide, hidden = x_ref.shape[2], gate_ref.shape[1]
    ring_at = lax.axis_index("ma_0")
    copies = []
    for k, (owner, block) in enumerate(zip(owners, blocks)):
        slot = lax.rem(ring_at + owner, RING)
        row = pl.ds(pl.multiple_of(slot * wide, wide), wide)
        copies.append(pltpu.make_async_copy(block, x_ref.at[k], x_sem.at[k]))
        sources = [
            gate_ref.at[row, :],
            up_ref.at[row, :],
            other_ref.at[slot, pl.ds(0, wide), :],
            other_ref.at[slot, pl.ds(wide, wide), :],
        ]
        for n, source in enumerate(sources):
            copies.append(
                pltpu.make_async_copy(
                    source, w_ref.at[k, :, pl.ds(n * hidden, hidden)], w_sem.at[k, n]
                )
            )
    return copies


def gate_kernel(owners, more, *refs):
    count = len(owners)
    blocks = refs[:count]
    gate_ref, up_ref, other_ref = refs[count : count + 3]
    refs = refs[count + 3 :]
    if more:
        acc_in_ref, squares_in_ref, refs = refs[0], refs[1], refs[2:]
    acc_ref, squares_ref, x_ref, w_ref, x_sem, w_sem = refs
    length = acc_ref.shape[0]
    copies = gate_copies(owners, blocks, gate_ref, up_ref, other_ref, x_ref, w_ref, x_sem, w_sem)
    for copy in copies:
        copy.start()
    if more:
        acc_ref[...] = acc_in_ref[...]
        squares_ref[...] = squares_in_ref[...]
    else:
        acc_ref[...] = jnp.zeros_like(acc_ref)
        squares_ref[...] = jnp.zeros_like(squares_ref)
    for copy in copies:
        copy.wait()

    def add_block(k, unused):
        squares_ref[...] += x_ref[k, length : length + 8, :length].astype(jnp.float32)
        acc_ref[...] += dot(x_ref[k, :length, :], w_ref[k])
        return unused

    lax.fori_loop(0, count, add_block, 0)


def hidden_kernel(width, *refs):
    count = len(LAST)
    blocks = refs[:count]
    gate_ref, up_ref, other_ref, acc_in_ref, squares_in_ref = refs[count : count + 5]
    hidden_ref, x_ref, w_ref, x_sem, w_sem = refs[count + 5 :]
    size = gate_ref.shape[1]
    length = hidden_ref.shape[0]
    copies = gate_copies(LAST, blocks, gate_ref, up_ref, other_ref, x_ref, w_ref, x_sem, w_sem)
    for copy in copies:
        copy.start()
    for copy in copies:
        copy.wait()
    rows = x_ref[0, :length, :]
    squares = squares_in_ref[0:1, :] + x_ref[0, length : length + 1, :length].astype(jnp.float32)
    scale = as_column(lax.rsqrt(squares / width + epsilon))
    for k in range(2):
        sums = []
        for n in (2 * k, 2 * k + 1):
            at = slice(n * size, (n + 1) * size)
            sums.append((acc_in_ref[:, at] + dot(rows, w_ref[0, :, at])) * scale)
        hidden_ref[:, k * size : (k + 1) * size] = (
            jax.nn.gelu(sums[0], approximate=True) * sums[1]
        ).astype(jnp.bfloat16)


def down_copies(owners, down_ref, other_ref, d_ref, d_sem):
    ring_at, pair_at = lax.axis_index("ma_0"), lax.axis_index("ma_1")
    part = d_ref.shape[2]
    size = down_ref.shape[0]
    copies = []
    for j, owner in enumerate(owners):
        slot = lax.rem(ring_at + owner, RING)
        column = pl.multiple_of((slot * 2 + pair_at) * part, part)
        sources = [down_ref.at[:, pl.ds(column, part)]]
        sources += [other_ref.at[slot, pl.ds(n * size, size), :] for n in (4, 6, 5)]
        for n, source in enumerate(sources):
            copies.append(
                pltpu.make_async_copy(source, d_ref.at[j, pl.ds(n * size, size), :], d_sem.at[j, n])
            )
    return copies


def down_kernel(owners, mine_ref, theirs_ref, down_ref, other_ref, *refs):
    *out_refs, h_ref, d_ref, h_sem, d_sem = refs
    copies = [
        pltpu.make_async_copy(ref, h_ref.at[k], h_sem.at[k])
        for k, ref in enumerate((mine_ref, theirs_ref))
    ] + down_copies(owners, down_ref, other_ref, d_ref, d_sem)
    for copy in copies:
        copy.start()
    for copy in copies:
        copy.wait()
    rows = h_ref.shape[2]

    def block(j):
        product = dot(h_ref[0], d_ref[j, :rows, :]) + dot(h_ref[1], d_ref[j, rows:, :])
        return product.astype(jnp.bfloat16)

    if len(out_refs) > 1:
        for j, out_ref in enumerate(out_refs):
            out_ref[...] = block(j)
        return

    def store(j, unused):
        out_refs[0][j] = block(j)
        return unused

    lax.fori_loop(0, len(owners), store, 0)


def feed_forward(held, gate, up, down, other):
    rows, wide = held[0].shape
    hidden = gate.shape[1]
    length = rows - 8
    part = wide // 2
    sums = [
        jax.ShapeDtypeStruct((length, 4 * hidden), jnp.float32),
        jax.ShapeDtypeStruct((8, length), jnp.float32),
    ]

    def scratch(count):
        return [
            pltpu.VMEM((count, rows, wide), jnp.bfloat16),
            pltpu.VMEM((count, wide, 4 * hidden), jnp.bfloat16),
            pltpu.SemaphoreType.DMA((count,)),
            pltpu.SemaphoreType.DMA((count, 4)),
        ]

    def cost(count, extra=0):
        return pl.CostEstimate(
            flops=2 * length * wide * 4 * hidden * count + extra,
            bytes_accessed=10**6 * (count + 1),
            transcendentals=0,
        )

    def gate_sums(owners, before):
        return pl.pallas_call(
            functools.partial(gate_kernel, owners, bool(before)),
            in_specs=[ANY] * (len(owners) + 3) + [IN_VMEM] * len(before),
            out_specs=[IN_VMEM] * 2,
            scratch_shapes=scratch(len(owners)),
            out_shape=sums,
            cost_estimate=cost(len(owners)),
        )(*[held[k] for k in owners], gate, up, other, *before)

    before = gate_sums(FIRST, ())
    before = gate_sums(SECOND, before)
    before = gate_sums(THIRD, before)
    mine = pl.pallas_call(
        functools.partial(hidden_kernel, float(wide * RING)),
        in_specs=[ANY] * (len(LAST) + 3) + [IN_VMEM] * 2,
        out_specs=IN_VMEM,
        scratch_shapes=scratch(len(LAST)),
        out_shape=jax.ShapeDtypeStruct((length, 2 * hidden), jnp.bfloat16),
        cost_estimate=cost(1),
        name="hidden",
    )(*[held[k] for k in LAST], gate, up, other, *before)
    theirs = lax.ppermute(mine, "ma_1", SWAP)

    def down_blocks(owners, shapes):
        return pl.pallas_call(
            functools.partial(down_kernel, owners),
            in_specs=[ANY] * 4,
            out_specs=[IN_VMEM] * len(shapes),
            scratch_shapes=[
                pltpu.VMEM((2, length, 2 * hidden), jnp.bfloat16),
                pltpu.VMEM((len(owners), 4 * hidden, part), jnp.bfloat16),
                pltpu.SemaphoreType.DMA((2,)),
                pltpu.SemaphoreType.DMA((len(owners), 4)),
            ],
            out_shape=shapes,
            cost_estimate=cost(1),
        )(mine, theirs, down, other)

    first, second = down_blocks(SEND[:2], [one_block(length, part)] * 2)
    (rest,) = down_blocks(SEND[2:], [rest_blocks(length, part)])
    return first, second, rest


def spread(values, gain):
    rows, width = values.shape
    as_float = values.astype(jnp.float32)
    squares = jnp.sum(as_float * as_float, axis=1)
    gained = (as_float * gain.astype(jnp.float32)).astype(jnp.bfloat16)
    line = jnp.concatenate([squares, jnp.zeros((width - rows,), jnp.float32)])
    tail = jnp.broadcast_to(line.astype(jnp.bfloat16)[None], (8, width))
    block = jnp.concatenate([gained, tail], axis=0)
    return ring_gather(block)


def layer(
    tokens,
    attn_gain,
    query_weight,
    key_weight,
    value_projection_matrix,
    attention_output_matrix,
    bucket_bias_matrix,
    ffn_gain,
    gate_weight,
    up_weight,
    down_projection_weight,
):
    sequences, length, part = tokens.shape
    copy_at = lax.axis_index("ba")
    copies = lax.axis_size("ba")
    token_rows = tokens.reshape(length, part)

    gains = jnp.concatenate(
        [attn_gain[None], ffn_gain[None], jnp.zeros((6, part), jnp.bfloat16)], axis=0
    )
    mine = jnp.concatenate([token_rows, gains], axis=0)
    theirs = lax.ppermute(mine, "ma_1", SWAP)

    half_rows = query_weight.shape[0]
    depth = half_rows // copies
    share = [
        lax.dynamic_slice_in_dim(w, copy_at * depth, depth, 0)
        for w in (query_weight, key_weight, value_projection_matrix)
    ]
    first_share = lax.ppermute(jnp.concatenate(share, axis=1), "row", SWAP)
    other_first = lax.all_gather(first_share, "ba", axis=0, tiled=True)
    gate_depth = gate_weight.shape[0] // copies
    gate_share = [
        lax.dynamic_slice_in_dim(w, copy_at * gate_depth, gate_depth, 0)
        for w in (gate_weight, up_weight)
    ]
    down_width = down_projection_weight.shape[1] // copies
    pair_at = lax.axis_index("ma_1")

    def down_share(pair):
        at = copy_at * down_width + pair * part
        return lax.dynamic_slice_in_dim(down_projection_weight, at, part, 1)

    wide = pair_order(mine, theirs, 1)
    wide_tokens = wide[:length]
    wide_attn_gain = wide[length]
    wide_ffn_gain = wide[length + 1]

    held = spread(wide_tokens, wide_attn_gain)
    core_width = attention_output_matrix.shape[1] // 2
    core_out = lax.dynamic_slice_in_dim(
        attention_output_matrix, jnp.mod(copy_at, 2) * core_width, core_width, 1
    )
    core_out = lax.ppermute(tied(core_out, held[1]), "row", SWAP)
    cores = [(k, k ^ 1) for k in range(copies)]
    other_core_out = lax.ppermute(core_out, "ba", cores)
    pair_share = tied(down_share(1 - pair_at), held[1])
    pair_share = lax.ppermute(pair_share, "ma_1", SWAP)
    row_share = jnp.concatenate([*gate_share, down_share(pair_at), pair_share], axis=0)
    row_share = lax.ppermute(tied(row_share, held[2]), "row", SWAP)
    out_blocks = attention(
        held,
        position_bias(bucket_bias_matrix, length),
        (query_weight, key_weight, value_projection_matrix),
        other_first,
        (attention_output_matrix, core_out, other_core_out),
    )
    row_share = tied(row_share, out_blocks[0])
    second_share = jnp.concatenate([row_share, pair_share], axis=0)
    other_second = lax.all_gather(second_share, "ba", axis=0, tiled=False)
    summed = ring_sum(*out_blocks).astype(jnp.bfloat16)
    partner = lax.ppermute(summed, "ma_1", SWAP)
    attn_out = summed.astype(jnp.float32) + partner.astype(jnp.float32)
    residual = (wide_tokens.astype(jnp.float32) + attn_out).astype(jnp.bfloat16)
    first = lax.axis_index("ma_1") == 0
    own_residual = jnp.where(first, residual[:, :part], residual[:, part:])

    held = spread(residual, wide_ffn_gain)
    summed = ring_sum(
        *feed_forward(held, gate_weight, up_weight, down_projection_weight, other_second),
    )
    encoded = own_residual.astype(jnp.float32) + summed
    return encoded.astype(jnp.bfloat16).reshape(sequences, length, part)


def solution(mesh):
    split = Mesh(
        mesh.devices.reshape(mesh.shape["ba"], RING, 2, mesh.shape["row"]),
        ("ba", "ma_0", "ma_1", "row"),
    )
    return jax.shard_map(
        layer,
        mesh=split,
        in_specs=(
            P(("ba", "row"), None, MA),
            P(MA),
            P("row", MA),
            P("row", MA),
            P("row", MA),
            P(MA, "row"),
            P(None, MA),
            P(MA),
            P(None, MA_ROW),
            P(None, MA_ROW),
            P(MA_ROW, None),
        ),
        out_specs=P(("ba", "row"), None, MA),
        check_vma=False,
    )
```

```python
import functools

import jax
import jax.numpy as jnp
from jax import lax
from jax.experimental import pallas as pl
from jax.experimental.pallas import tpu as pltpu
from jax.sharding import Mesh
from jax.sharding import PartitionSpec as P

MA = ("ma_0", "ma_1")
MA_ROW = ("ma_0", "ma_1", "row")

bucket_thresholds = (1, 2, 3, 4, 5, 6, 7, 8, 11, 16, 23, 32, 45, 64, 91, 128)
epsilon = 1e-06
RING = 8
SWAP = [(0, 1), (1, 0)]
UP = [(i, (i + 1) % RING) for i in range(RING)]
DOWN = [(i, (i - 1) % RING) for i in range(RING)]


def tied(value, *after):
    return lax.optimization_barrier((value, *after))[0]


def pair_order(mine, theirs, axis):
    first = lax.axis_index("ma_1") == 0
    return jnp.where(
        first,
        jnp.concatenate([mine, theirs], axis=axis),
        jnp.concatenate([theirs, mine], axis=axis),
    )


def ring_gather(block):
    held = {0: block}
    above = below = block
    for step in range(1, RING // 2 + 1):
        above = lax.ppermute(above, "ma_0", DOWN)
        held[step] = above
        if step < RING // 2:
            below = lax.ppermute(below, "ma_0", UP)
            held[RING - step] = below
    return held


SEND = (4, 5, 0, 1, 2, 3, 6, 7)


def ring_sum(first, second, rest):
    blocks = [first, second, *(rest[k] for k in range(RING - 2))]

    def block(owner):
        return blocks[SEND.index(owner % RING)].astype(jnp.float32)

    up, down = blocks[0], blocks[1]
    got_down = None
    for step in range(1, RING // 2 + 1):
        got_up = lax.ppermute(up, "ma_0", UP)
        if step > 1:
            got_down = lax.ppermute(down, "ma_0", DOWN)
        if step < RING // 2:
            up = (got_up.astype(jnp.float32) + block(4 - step)).astype(jnp.bfloat16)
            if got_down is not None:
                down = (got_down.astype(jnp.float32) + block(step - 4)).astype(jnp.bfloat16)
    return got_up.astype(jnp.float32) + got_down.astype(jnp.float32) + block(0)


def bias_kernel(bucket_ref, table_ref, bias_ref):
    heads, rows, columns = bias_ref.shape
    bucket = bucket_ref[...]
    lines = jnp.zeros(bucket.shape, jnp.float32)
    for b in range(table_ref.shape[1]):
        lines = jnp.where(bucket == b, table_ref[:, b : b + 1], lines)
    for h in range(heads):
        wide = jnp.broadcast_to(lines[h : h + 1, :], (rows, bucket.shape[1]))
        bias_ref[h] = pltpu.roll(wide, 0, 1, stride=1, stride_axis=0)[:, :columns]


def position_bias(table, length):
    offset = jnp.arange(2 * length, dtype=jnp.int32)
    offset = jnp.where(offset < length, offset, offset - 2 * length)
    distance = jnp.abs(offset)
    bucket = jnp.where(offset > 0, 15, 0)
    for threshold in bucket_thresholds[:15]:
        bucket = bucket + (distance >= threshold).astype(jnp.int32)
    last = (distance >= bucket_thresholds[15]) & (offset > 0)
    bucket = bucket + last.astype(jnp.int32)
    heads = table.shape[1]
    return pl.pallas_call(
        bias_kernel,
        out_shape=jax.ShapeDtypeStruct((heads, length, length), jnp.float32),
        cost_estimate=pl.CostEstimate(flops=10**8, bytes_accessed=10**6, transcendentals=0),
        name="position_bias",
    )(jnp.broadcast_to(bucket[None], (heads, 2 * length)), table.T)


def as_column(line):
    size = line.shape[1]
    at_row = lax.broadcasted_iota(jnp.int32, (size, size), 0)
    at_column = lax.broadcasted_iota(jnp.int32, (size, size), 1)
    spread_out = jnp.where(at_row == at_column, jnp.broadcast_to(line, (size, size)), 0.0)
    return jnp.sum(spread_out, axis=1, keepdims=True)


def dot(a, b):
    return jnp.dot(a, b, preferred_element_type=jnp.float32)


def attention_kernel(width, *refs):
    ring_at, half = lax.axis_index("ma_0"), lax.axis_index("row")
    blocks = refs[:RING]
    own = refs[RING : RING + 3]
    other_ref, *out_weight_refs, bias_ref = refs[RING + 3 : RING + 8]
    first_ref, second_ref, attended_ref = refs[RING + 8 : RING + 11]
    x_ref, w_ref, o_ref, acc_ref, both_ref, table_ref = refs[RING + 11 : RING + 17]
    x_sem, own_sem, other_sem, o_sem, table_sem = refs[RING + 17 :]
    table_copy = pltpu.make_async_copy(bias_ref, table_ref, table_sem)
    length = acc_ref.shape[0]
    inner = attended_ref.shape[1]
    wide = x_ref.shape[2]
    parts = RING // 2
    rows = parts * wide

    own_copies = [
        pltpu.make_async_copy(
            own[k], w_ref.at[pl.ds(0, rows), pl.ds(k * inner, inner)], own_sem.at[k]
        )
        for k in range(3)
    ]
    x_copies = [
        pltpu.make_async_copy(blocks[k], x_ref.at[k], x_sem.at[k]) for k in range(RING)
    ]
    other_copies = [
        pltpu.make_async_copy(
            other_ref.at[pl.ds(k * wide, wide), :],
            w_ref.at[pl.ds(rows + k * wide, wide), :],
            other_sem.at[k],
        )
        for k in range(parts)
    ]
    o_copies = out_weight_copies(out_weight_refs, o_ref, o_sem)
    for copy in x_copies + own_copies + other_copies + [table_copy] + o_copies:
        copy.start()
    for copy in x_copies:
        copy.wait()
    squares = x_ref[0, length : length + 1, :length].astype(jnp.float32)
    for k in range(1, RING):
        squares += x_ref[k, length : length + 1, :length].astype(jnp.float32)
    scale = as_column(lax.rsqrt(squares / width + epsilon))
    for copy in own_copies:
        copy.wait()
    acc_ref[...] = jnp.zeros_like(acc_ref)

    def add_slot(slot, unused):
        weights = w_ref[pl.ds(pl.multiple_of(slot * wide, wide), wide), :]
        block = lax.rem(slot + half * parts + RING - ring_at, RING)
        acc_ref[...] += dot(x_ref[block, :length, :], weights)
        return unused

    lax.fori_loop(0, parts, add_slot, 0)
    for copy in other_copies:
        copy.wait()
    lax.fori_loop(parts, RING, add_slot, 0)

    heads = bias_ref.shape[0]
    size = inner // heads
    pair = 2 * size

    table_copy.wait()

    def two_heads(n, unused):
        query, key, value = (
            (acc_ref[:, pl.ds(pl.multiple_of(k * inner + n * pair, pair), pair)] * scale).astype(
                jnp.bfloat16
            )
            for k in range(3)
        )
        for h in range(2):
            at = slice(h * size, (h + 1) * size)
            scores = (
                lax.dot_general(
                    query[:, at],
                    key[:, at],
                    (((1,), (1,)), ((), ())),
                    preferred_element_type=jnp.float32,
                )
                + table_ref[2 * n + h]
            )
            exponent = jnp.exp(scores - jnp.max(scores, axis=-1, keepdims=True))
            weights = exponent / jnp.sum(exponent, axis=-1, keepdims=True)
            both_ref[:, at] = dot(weights.astype(jnp.bfloat16), value[:, at]).astype(jnp.bfloat16)
        attended_ref[:, pl.ds(pl.multiple_of(n * pair, pair), pair)] = both_ref[...]
        return unused

    lax.fori_loop(0, heads // 2, two_heads, 0)

    for copy in o_copies:
        copy.wait()

    first_ref[...] = out_block(SEND[0], attended_ref, o_ref)
    second_ref[...] = out_block(SEND[1], attended_ref, o_ref)


def out_weight_copies(refs, o_ref, o_sem):
    width = refs[1].shape[1]
    core = lax.rem(lax.axis_index("ba"), 2)
    targets = [
        o_ref.at[0],
        o_ref.at[1, :, pl.ds(pl.multiple_of(core * width, width), width)],
        o_ref.at[1, :, pl.ds(pl.multiple_of((1 - core) * width, width), width)],
    ]
    return [
        pltpu.make_async_copy(ref, target, o_sem.at[k])
        for k, (ref, target) in enumerate(zip(refs, targets))
    ]


def out_block(owner, attended_ref, o_ref):
    ring_at, half = lax.axis_index("ma_0"), lax.axis_index("row")
    parts = RING // 2
    wide = o_ref.shape[2] // parts
    slot = lax.rem(ring_at + owner + half * parts, RING)
    which = slot // parts
    column = pl.multiple_of((slot - which * parts) * wide, wide)
    product = dot(attended_ref[...], o_ref[which, :, pl.ds(column, wide)])
    return product.astype(jnp.bfloat16)


def out_rest_kernel(*refs):
    out_weight_refs = refs[1:4]
    rest_ref, o_ref, o_sem, attended_ref, attended_sem = refs[4:]
    copies = [pltpu.make_async_copy(refs[0], attended_ref, attended_sem)]
    copies += out_weight_copies(out_weight_refs, o_ref, o_sem)
    for copy in copies:
        copy.start()
    for copy in copies:
        copy.wait()
    store_rest(lambda owner: out_block(owner, attended_ref, o_ref), rest_ref)


def store_rest(block, rest_ref):
    def store(k, unused):
        rest_ref[k] = block(jnp.where(k < 4, k, k + 2))
        return unused

    lax.fori_loop(0, RING - 2, store, 0)


def one_block(length, width):
    return jax.ShapeDtypeStruct((length, width), jnp.bfloat16)


def rest_blocks(length, width):
    return jax.ShapeDtypeStruct((RING - 2, length, width), jnp.bfloat16)


ANY = pl.BlockSpec(memory_space=pl.ANY)
IN_VMEM = pl.BlockSpec(memory_space=pltpu.VMEM)


def attention(held, bias, own, other, out_weights):
    length = bias.shape[1]
    inner = own[0].shape[1]
    rows, wide = held[0].shape
    parts = RING // 2
    out_scratch = [
        pltpu.VMEM((2, *out_weights[0].shape), jnp.bfloat16),
        pltpu.SemaphoreType.DMA((3,)),
    ]
    first, second, attended = pl.pallas_call(
        functools.partial(attention_kernel, float(wide * RING)),
        in_specs=[ANY] * (RING + 8),
        out_specs=[IN_VMEM] * 3,
        scratch_shapes=[
            pltpu.VMEM((RING, rows, wide), jnp.bfloat16),
            pltpu.VMEM((RING * wide, 3 * inner), jnp.bfloat16),
            out_scratch[0],
            pltpu.VMEM((length, 3 * inner), jnp.float32),
            pltpu.VMEM((length, 2 * inner // bias.shape[0]), jnp.bfloat16),
            pltpu.VMEM(bias.shape, jnp.float32),
            pltpu.SemaphoreType.DMA((RING,)),
            pltpu.SemaphoreType.DMA((3,)),
            pltpu.SemaphoreType.DMA((parts,)),
            out_scratch[1],
            pltpu.SemaphoreType.DMA,
        ],
        out_shape=[one_block(length, wide)] * 2 + [one_block(length, inner)],
        cost_estimate=pl.CostEstimate(
            flops=2 * length * wide * RING * 4 * inner, bytes_accessed=10**7, transcendentals=0
        ),
        name="attention",
    )(
        *[held[k] for k in range(RING)],
        *own,
        other,
        *out_weights,
        bias,
    )
    rest = pl.pallas_call(
        out_rest_kernel,
        in_specs=[ANY] * 4,
        out_specs=IN_VMEM,
        scratch_shapes=out_scratch
        + [pltpu.VMEM((length, inner), jnp.bfloat16), pltpu.SemaphoreType.DMA],
        out_shape=rest_blocks(length, wide),
        cost_estimate=pl.CostEstimate(
            flops=2 * length * inner * wide * (RING - 2),
            bytes_accessed=4 * 10**6,
            transcendentals=0,
        ),
        name="out_rest",
    )(attended, *out_weights)
    return first, second, rest


FIRST = (0, 1, 7)
SECOND = (2, 6)
THIRD = (3, 5)
LAST = (4,)


def gate_copies(owners, blocks, gate_ref, up_ref, other_ref, x_ref, w_ref, x_sem, w_sem):
    wide, hidden = x_ref.shape[2], gate_ref.shape[1]
    ring_at = lax.axis_index("ma_0")
    copies = []
    for k, (owner, block) in enumerate(zip(owners, blocks)):
        slot = lax.rem(ring_at + owner, RING)
        row = pl.ds(pl.multiple_of(slot * wide, wide), wide)
        copies.append(pltpu.make_async_copy(block, x_ref.at[k], x_sem.at[k]))
        sources = [
            gate_ref.at[row, :],
            up_ref.at[row, :],
            other_ref.at[slot, pl.ds(0, wide), :],
            other_ref.at[slot, pl.ds(wide, wide), :],
        ]
        for n, source in enumerate(sources):
            copies.append(
                pltpu.make_async_copy(
                    source, w_ref.at[k, :, pl.ds(n * hidden, hidden)], w_sem.at[k, n]
                )
            )
    return copies


def gate_kernel(owners, more, *refs):
    count = len(owners)
    blocks = refs[:count]
    gate_ref, up_ref, other_ref = refs[count : count + 3]
    refs = refs[count + 3 :]
    if more:
        acc_in_ref, squares_in_ref, refs = refs[0], refs[1], refs[2:]
    acc_ref, squares_ref, x_ref, w_ref, x_sem, w_sem, sum_sem = refs
    length = acc_ref.shape[0]
    copies = gate_copies(owners, blocks, gate_ref, up_ref, other_ref, x_ref, w_ref, x_sem, w_sem)
    if more:
        copies.append(pltpu.make_async_copy(squares_in_ref, squares_ref, sum_sem.at[0]))
        copies.append(pltpu.make_async_copy(acc_in_ref, acc_ref, sum_sem.at[1]))
    for copy in copies:
        copy.start()
    if not more:
        acc_ref[...] = jnp.zeros_like(acc_ref)
        squares_ref[...] = jnp.zeros_like(squares_ref)
    for copy in copies:
        copy.wait()

    def add_block(k, unused):
        squares_ref[...] += x_ref[k, length : length + 8, :length].astype(jnp.float32)
        acc_ref[...] += dot(x_ref[k, :length, :], w_ref[k])
        return unused

    lax.fori_loop(0, count, add_block, 0)


def hidden_kernel(width, *refs):
    count = len(LAST)
    blocks = refs[:count]
    gate_ref, up_ref, other_ref, acc_in_ref, squares_in_ref = refs[count : count + 5]
    hidden_ref, x_ref, w_ref, x_sem, w_sem, sum_sem, acc_ref, squares_ref = refs[count + 5 :]
    size = gate_ref.shape[1]
    length = hidden_ref.shape[0]
    copies = gate_copies(LAST, blocks, gate_ref, up_ref, other_ref, x_ref, w_ref, x_sem, w_sem)
    copies.append(pltpu.make_async_copy(squares_in_ref, squares_ref, sum_sem.at[0]))
    copies.append(pltpu.make_async_copy(acc_in_ref, acc_ref, sum_sem.at[1]))
    for copy in copies:
        copy.start()
    for copy in copies:
        copy.wait()
    rows = x_ref[0, :length, :]
    squares = squares_ref[0:1, :] + x_ref[0, length : length + 1, :length].astype(jnp.float32)
    scale = as_column(lax.rsqrt(squares / width + epsilon))
    for k in range(2):
        sums = []
        for n in (2 * k, 2 * k + 1):
            at = slice(n * size, (n + 1) * size)
            sums.append((acc_ref[:, at] + dot(rows, w_ref[0, :, at])) * scale)
        hidden_ref[:, k * size : (k + 1) * size] = (
            jax.nn.gelu(sums[0], approximate=True) * sums[1]
        ).astype(jnp.bfloat16)


def down_copies(owners, down_ref, other_ref, d_ref, d_sem):
    ring_at, pair_at = lax.axis_index("ma_0"), lax.axis_index("ma_1")
    part = d_ref.shape[2]
    size = down_ref.shape[0]
    copies = []
    for j, owner in enumerate(owners):
        slot = lax.rem(ring_at + owner, RING)
        column = pl.multiple_of((slot * 2 + pair_at) * part, part)
        sources = [down_ref.at[:, pl.ds(column, part)]]
        sources += [other_ref.at[slot, pl.ds(n * size, size), :] for n in (4, 6, 5)]
        for n, source in enumerate(sources):
            copies.append(
                pltpu.make_async_copy(source, d_ref.at[j, pl.ds(n * size, size), :], d_sem.at[j, n])
            )
    return copies


def down_kernel(owners, mine_ref, theirs_ref, down_ref, other_ref, *refs):
    *out_refs, h_ref, d_ref, h_sem, d_sem = refs
    copies = [
        pltpu.make_async_copy(ref, h_ref.at[k], h_sem.at[k])
        for k, ref in enumerate((mine_ref, theirs_ref))
    ] + down_copies(owners, down_ref, other_ref, d_ref, d_sem)
    for copy in copies:
        copy.start()
    for copy in copies:
        copy.wait()
    rows = h_ref.shape[2]

    def block(j):
        product = dot(h_ref[0], d_ref[j, :rows, :]) + dot(h_ref[1], d_ref[j, rows:, :])
        return product.astype(jnp.bfloat16)

    if len(out_refs) > 1:
        for j, out_ref in enumerate(out_refs):
            out_ref[...] = block(j)
        return

    def store(j, unused):
        out_refs[0][j] = block(j)
        return unused

    lax.fori_loop(0, len(owners), store, 0)


def feed_forward(held, gate, up, down, other):
    rows, wide = held[0].shape
    hidden = gate.shape[1]
    length = rows - 8
    part = wide // 2
    sums = [
        jax.ShapeDtypeStruct((length, 4 * hidden), jnp.float32),
        jax.ShapeDtypeStruct((8, length), jnp.float32),
    ]

    def scratch(count):
        return [
            pltpu.VMEM((count, rows, wide), jnp.bfloat16),
            pltpu.VMEM((count, wide, 4 * hidden), jnp.bfloat16),
            pltpu.SemaphoreType.DMA((count,)),
            pltpu.SemaphoreType.DMA((count, 4)),
            pltpu.SemaphoreType.DMA((2,)),
        ]

    def cost(count, extra=0):
        return pl.CostEstimate(
            flops=2 * length * wide * 4 * hidden * count + extra,
            bytes_accessed=10**6 * (count + 1),
            transcendentals=0,
        )

    def gate_sums(owners, before):
        return pl.pallas_call(
            functools.partial(gate_kernel, owners, bool(before)),
            in_specs=[ANY] * (len(owners) + 3 + len(before)),
            out_specs=[IN_VMEM] * 2,
            scratch_shapes=scratch(len(owners)),
            out_shape=sums,
            cost_estimate=cost(len(owners)),
        )(*[held[k] for k in owners], gate, up, other, *before)

    before = gate_sums(FIRST, ())
    before = gate_sums(SECOND, before)
    before = gate_sums(THIRD, before)
    mine = pl.pallas_call(
        functools.partial(hidden_kernel, float(wide * RING)),
        in_specs=[ANY] * (len(LAST) + 5),
        out_specs=IN_VMEM,
        scratch_shapes=scratch(len(LAST)) + [pltpu.VMEM(s.shape, s.dtype) for s in sums],
        out_shape=jax.ShapeDtypeStruct((length, 2 * hidden), jnp.bfloat16),
        cost_estimate=cost(1),
        name="hidden",
    )(*[held[k] for k in LAST], gate, up, other, *before)
    theirs = lax.ppermute(mine, "ma_1", SWAP)

    def down_blocks(owners, shapes):
        return pl.pallas_call(
            functools.partial(down_kernel, owners),
            in_specs=[ANY] * 4,
            out_specs=[IN_VMEM] * len(shapes),
            scratch_shapes=[
                pltpu.VMEM((2, length, 2 * hidden), jnp.bfloat16),
                pltpu.VMEM((len(owners), 4 * hidden, part), jnp.bfloat16),
                pltpu.SemaphoreType.DMA((2,)),
                pltpu.SemaphoreType.DMA((len(owners), 4)),
            ],
            out_shape=shapes,
            cost_estimate=cost(1),
        )(mine, theirs, down, other)

    first, second = down_blocks(SEND[:2], [one_block(length, part)] * 2)
    (rest,) = down_blocks(SEND[2:], [rest_blocks(length, part)])
    return first, second, rest


def spread(values, gain):
    rows, width = values.shape
    as_float = values.astype(jnp.float32)
    squares = jnp.sum(as_float * as_float, axis=1)
    gained = (as_float * gain.astype(jnp.float32)).astype(jnp.bfloat16)
    line = jnp.concatenate([squares, jnp.zeros((width - rows,), jnp.float32)])
    tail = jnp.broadcast_to(line.astype(jnp.bfloat16)[None], (8, width))
    block = jnp.concatenate([gained, tail], axis=0)
    return ring_gather(block)


def layer(
    tokens,
    attn_gain,
    query_weight,
    key_weight,
    value_projection_matrix,
    attention_output_matrix,
    bucket_bias_matrix,
    ffn_gain,
    gate_weight,
    up_weight,
    down_projection_weight,
):
    sequences, length, part = tokens.shape
    copy_at = lax.axis_index("ba")
    copies = lax.axis_size("ba")
    token_rows = tokens.reshape(length, part)

    gains = jnp.concatenate(
        [attn_gain[None], ffn_gain[None], jnp.zeros((6, part), jnp.bfloat16)], axis=0
    )
    mine = jnp.concatenate([token_rows, gains], axis=0)
    theirs = lax.ppermute(mine, "ma_1", SWAP)

    half_rows = query_weight.shape[0]
    depth = half_rows // copies
    share = [
        lax.dynamic_slice_in_dim(w, copy_at * depth, depth, 0)
        for w in (query_weight, key_weight, value_projection_matrix)
    ]
    first_share = lax.ppermute(jnp.concatenate(share, axis=1), "row", SWAP)
    other_first = lax.all_gather(first_share, "ba", axis=0, tiled=True)
    gate_depth = gate_weight.shape[0] // copies
    gate_share = [
        lax.dynamic_slice_in_dim(w, copy_at * gate_depth, gate_depth, 0)
        for w in (gate_weight, up_weight)
    ]
    down_width = down_projection_weight.shape[1] // copies
    pair_at = lax.axis_index("ma_1")

    def down_share(pair):
        at = copy_at * down_width + pair * part
        return lax.dynamic_slice_in_dim(down_projection_weight, at, part, 1)

    wide = pair_order(mine, theirs, 1)
    wide_tokens = wide[:length]
    wide_attn_gain = wide[length]
    wide_ffn_gain = wide[length + 1]

    held = spread(wide_tokens, wide_attn_gain)
    core_width = attention_output_matrix.shape[1] // 2
    core_out = lax.dynamic_slice_in_dim(
        attention_output_matrix, jnp.mod(copy_at, 2) * core_width, core_width, 1
    )
    core_out = lax.ppermute(tied(core_out, held[1]), "row", SWAP)
    cores = [(k, k ^ 1) for k in range(copies)]
    other_core_out = lax.ppermute(core_out, "ba", cores)
    pair_share = tied(down_share(1 - pair_at), held[1])
    pair_share = lax.ppermute(pair_share, "ma_1", SWAP)
    pair_share = tied(pair_share, held[3])
    same_share = down_share(pair_at)
    row_share = jnp.concatenate([*gate_share, same_share, pair_share], axis=0)
    row_share = lax.ppermute(row_share, "row", SWAP)
    out_blocks = attention(
        held,
        position_bias(bucket_bias_matrix, length),
        (query_weight, key_weight, value_projection_matrix),
        other_first,
        (attention_output_matrix, core_out, other_core_out),
    )
    row_share = tied(row_share, out_blocks[0])
    second_share = jnp.concatenate([row_share, pair_share], axis=0)
    other_second = lax.all_gather(second_share, "ba", axis=0, tiled=False)
    summed = ring_sum(*out_blocks).astype(jnp.bfloat16)
    partner = lax.ppermute(summed, "ma_1", SWAP)
    attn_out = summed.astype(jnp.float32) + partner.astype(jnp.float32)
    residual = (wide_tokens.astype(jnp.float32) + attn_out).astype(jnp.bfloat16)
    first = lax.axis_index("ma_1") == 0
    own_residual = jnp.where(first, residual[:, :part], residual[:, part:])

    held = spread(residual, wide_ffn_gain)
    summed = ring_sum(
        *feed_forward(held, gate_weight, up_weight, down_projection_weight, other_second),
    )
    encoded = own_residual.astype(jnp.float32) + summed
    return encoded.astype(jnp.bfloat16).reshape(sequences, length, part)


def solution(mesh):
    split = Mesh(
        mesh.devices.reshape(mesh.shape["ba"], RING, 2, mesh.shape["row"]),
        ("ba", "ma_0", "ma_1", "row"),
    )
    return jax.shard_map(
        layer,
        mesh=split,
        in_specs=(
            P(("ba", "row"), None, MA),
            P(MA),
            P("row", MA),
            P("row", MA),
            P("row", MA),
            P(MA, "row"),
            P(None, MA),
            P(MA),
            P(None, MA_ROW),
            P(None, MA_ROW),
            P(MA_ROW, None),
        ),
        out_specs=P(("ba", "row"), None, MA),
        check_vma=False,
    )
```

```python
import functools

import jax
import jax.numpy as jnp
from jax import lax
from jax.experimental import pallas as pl
from jax.experimental.pallas import tpu as pltpu
from jax.sharding import Mesh
from jax.sharding import PartitionSpec as P

MA = ("ma_0", "ma_1")
MA_ROW = ("ma_0", "ma_1", "row")

bucket_thresholds = (1, 2, 3, 4, 5, 6, 7, 8, 11, 16, 23, 32, 45, 64, 91, 128)
epsilon = 1e-06
RING = 8
SWAP = [(0, 1), (1, 0)]
UP = [(i, (i + 1) % RING) for i in range(RING)]
DOWN = [(i, (i - 1) % RING) for i in range(RING)]


def tied(value, *after):
    return lax.optimization_barrier((value, *after))[0]


def pair_order(mine, theirs, axis):
    first = lax.axis_index("ma_1") == 0
    return jnp.where(
        first,
        jnp.concatenate([mine, theirs], axis=axis),
        jnp.concatenate([theirs, mine], axis=axis),
    )


def ring_gather(block):
    held = {0: block}
    above = below = block
    for step in range(1, RING // 2 + 1):
        above = lax.ppermute(above, "ma_0", DOWN)
        held[step] = above
        if step < RING // 2:
            below = lax.ppermute(below, "ma_0", UP)
            held[RING - step] = below
    return held


SEND = (4, 5, 0, 1, 2, 3, 6, 7)


def ring_sum(first, second, rest):
    blocks = [first, second, *(rest[k] for k in range(RING - 2))]

    def block(owner):
        return blocks[SEND.index(owner % RING)].astype(jnp.float32)

    up, down = blocks[0], blocks[1]
    got_down = None
    for step in range(1, RING // 2 + 1):
        got_up = lax.ppermute(up, "ma_0", UP)
        if step > 1:
            got_down = lax.ppermute(down, "ma_0", DOWN)
        if step < RING // 2:
            up = (got_up.astype(jnp.float32) + block(4 - step)).astype(jnp.bfloat16)
            if got_down is not None:
                down = (got_down.astype(jnp.float32) + block(step - 4)).astype(jnp.bfloat16)
    return got_up.astype(jnp.float32) + got_down.astype(jnp.float32) + block(0)


def bias_kernel(bucket_ref, table_ref, bias_ref):
    heads, rows, columns = bias_ref.shape
    bucket = bucket_ref[...]
    lines = jnp.zeros(bucket.shape, jnp.float32)
    for b in range(table_ref.shape[1]):
        lines = jnp.where(bucket == b, table_ref[:, b : b + 1], lines)
    for h in range(heads):
        wide = jnp.broadcast_to(lines[h : h + 1, :], (rows, bucket.shape[1]))
        bias_ref[h] = pltpu.roll(wide, 0, 1, stride=1, stride_axis=0)[:, :columns]


def position_bias(table, length):
    offset = jnp.arange(2 * length, dtype=jnp.int32)
    offset = jnp.where(offset < length, offset, offset - 2 * length)
    distance = jnp.abs(offset)
    bucket = jnp.where(offset > 0, 15, 0)
    for threshold in bucket_thresholds[:15]:
        bucket = bucket + (distance >= threshold).astype(jnp.int32)
    last = (distance >= bucket_thresholds[15]) & (offset > 0)
    bucket = bucket + last.astype(jnp.int32)
    heads = table.shape[1]
    return pl.pallas_call(
        bias_kernel,
        out_shape=jax.ShapeDtypeStruct((heads, length, length), jnp.float32),
        cost_estimate=pl.CostEstimate(flops=10**8, bytes_accessed=10**6, transcendentals=0),
        name="position_bias",
    )(jnp.broadcast_to(bucket[None], (heads, 2 * length)), table.T)


def as_column(line):
    size = line.shape[1]
    at_row = lax.broadcasted_iota(jnp.int32, (size, size), 0)
    at_column = lax.broadcasted_iota(jnp.int32, (size, size), 1)
    spread_out = jnp.where(at_row == at_column, jnp.broadcast_to(line, (size, size)), 0.0)
    return jnp.sum(spread_out, axis=1, keepdims=True)


def dot(a, b):
    return jnp.dot(a, b, preferred_element_type=jnp.float32)


def attention_kernel(width, *refs):
    ring_at, half = lax.axis_index("ma_0"), lax.axis_index("row")
    blocks = refs[:RING]
    own = refs[RING : RING + 3]
    other_ref, *out_weight_refs, bias_ref = refs[RING + 3 : RING + 8]
    first_ref, second_ref, attended_ref = refs[RING + 8 : RING + 11]
    x_ref, w_ref, o_ref, acc_ref, both_ref, table_ref = refs[RING + 11 : RING + 17]
    x_sem, own_sem, other_sem, o_sem, table_sem = refs[RING + 17 :]
    table_copy = pltpu.make_async_copy(bias_ref, table_ref, table_sem)
    length = acc_ref.shape[0]
    inner = attended_ref.shape[1]
    wide = x_ref.shape[2]
    parts = RING // 2
    rows = parts * wide

    own_copies = [
        pltpu.make_async_copy(
            own[k], w_ref.at[pl.ds(0, rows), pl.ds(k * inner, inner)], own_sem.at[k]
        )
        for k in range(3)
    ]
    x_copies = [
        pltpu.make_async_copy(blocks[k], x_ref.at[k], x_sem.at[k]) for k in range(RING)
    ]
    other_copies = [
        pltpu.make_async_copy(
            other_ref.at[pl.ds(k * wide, wide), :],
            w_ref.at[pl.ds(rows + k * wide, wide), :],
            other_sem.at[k],
        )
        for k in range(parts)
    ]
    o_copies = out_weight_copies(out_weight_refs, o_ref, o_sem)
    for copy in x_copies + own_copies + other_copies + [table_copy] + o_copies:
        copy.start()
    for copy in x_copies:
        copy.wait()
    squares = x_ref[0, length : length + 1, :length].astype(jnp.float32)
    for k in range(1, RING):
        squares += x_ref[k, length : length + 1, :length].astype(jnp.float32)
    scale = as_column(lax.rsqrt(squares / width + epsilon))
    for copy in own_copies:
        copy.wait()
    acc_ref[...] = jnp.zeros_like(acc_ref)

    def add_slot(slot, unused):
        weights = w_ref[pl.ds(pl.multiple_of(slot * wide, wide), wide), :]
        block = lax.rem(slot + half * parts + RING - ring_at, RING)
        acc_ref[...] += dot(x_ref[block, :length, :], weights)
        return unused

    lax.fori_loop(0, parts, add_slot, 0)
    for copy in other_copies:
        copy.wait()
    lax.fori_loop(parts, RING, add_slot, 0)

    heads = bias_ref.shape[0]
    size = inner // heads
    pair = 2 * size

    table_copy.wait()

    def two_heads(n, unused):
        query, key, value = (
            (acc_ref[:, pl.ds(pl.multiple_of(k * inner + n * pair, pair), pair)] * scale).astype(
                jnp.bfloat16
            )
            for k in range(3)
        )
        for h in range(2):
            at = slice(h * size, (h + 1) * size)
            scores = (
                lax.dot_general(
                    query[:, at],
                    key[:, at],
                    (((1,), (1,)), ((), ())),
                    preferred_element_type=jnp.float32,
                )
                + table_ref[2 * n + h]
            )
            exponent = jnp.exp(scores - jnp.max(scores, axis=-1, keepdims=True))
            weights = exponent / jnp.sum(exponent, axis=-1, keepdims=True)
            both_ref[:, at] = dot(weights.astype(jnp.bfloat16), value[:, at]).astype(jnp.bfloat16)
        attended_ref[:, pl.ds(pl.multiple_of(n * pair, pair), pair)] = both_ref[...]
        return unused

    lax.fori_loop(0, heads // 2, two_heads, 0)

    for copy in o_copies:
        copy.wait()

    first_ref[...] = out_block(SEND[0], attended_ref, o_ref)
    second_ref[...] = out_block(SEND[1], attended_ref, o_ref)


def out_weight_copies(refs, o_ref, o_sem):
    width = refs[1].shape[1]
    core = lax.rem(lax.axis_index("ba"), 2)
    targets = [
        o_ref.at[0],
        o_ref.at[1, :, pl.ds(pl.multiple_of(core * width, width), width)],
        o_ref.at[1, :, pl.ds(pl.multiple_of((1 - core) * width, width), width)],
    ]
    return [
        pltpu.make_async_copy(ref, target, o_sem.at[k])
        for k, (ref, target) in enumerate(zip(refs, targets))
    ]


def out_block(owner, attended_ref, o_ref):
    ring_at, half = lax.axis_index("ma_0"), lax.axis_index("row")
    parts = RING // 2
    wide = o_ref.shape[2] // parts
    slot = lax.rem(ring_at + owner + half * parts, RING)
    which = slot // parts
    column = pl.multiple_of((slot - which * parts) * wide, wide)
    product = dot(attended_ref[...], o_ref[which, :, pl.ds(column, wide)])
    return product.astype(jnp.bfloat16)


def out_rest_kernel(*refs):
    out_weight_refs = refs[1:4]
    rest_ref, o_ref, o_sem, attended_ref, attended_sem = refs[4:]
    copies = [pltpu.make_async_copy(refs[0], attended_ref, attended_sem)]
    copies += out_weight_copies(out_weight_refs, o_ref, o_sem)
    for copy in copies:
        copy.start()
    for copy in copies:
        copy.wait()
    store_rest(lambda owner: out_block(owner, attended_ref, o_ref), rest_ref)


def store_rest(block, rest_ref):
    def store(k, unused):
        rest_ref[k] = block(jnp.where(k < 4, k, k + 2))
        return unused

    lax.fori_loop(0, RING - 2, store, 0)


def one_block(length, width):
    return jax.ShapeDtypeStruct((length, width), jnp.bfloat16)


def rest_blocks(length, width):
    return jax.ShapeDtypeStruct((RING - 2, length, width), jnp.bfloat16)


ANY = pl.BlockSpec(memory_space=pl.ANY)
IN_VMEM = pl.BlockSpec(memory_space=pltpu.VMEM)


def attention(held, bias, own, other, out_weights):
    length = bias.shape[1]
    inner = own[0].shape[1]
    rows, wide = held[0].shape
    parts = RING // 2
    out_scratch = [
        pltpu.VMEM((2, *out_weights[0].shape), jnp.bfloat16),
        pltpu.SemaphoreType.DMA((3,)),
    ]
    first, second, attended = pl.pallas_call(
        functools.partial(attention_kernel, float(wide * RING)),
        in_specs=[ANY] * (RING + 8),
        out_specs=[IN_VMEM] * 3,
        scratch_shapes=[
            pltpu.VMEM((RING, rows, wide), jnp.bfloat16),
            pltpu.VMEM((RING * wide, 3 * inner), jnp.bfloat16),
            out_scratch[0],
            pltpu.VMEM((length, 3 * inner), jnp.float32),
            pltpu.VMEM((length, 2 * inner // bias.shape[0]), jnp.bfloat16),
            pltpu.VMEM(bias.shape, jnp.float32),
            pltpu.SemaphoreType.DMA((RING,)),
            pltpu.SemaphoreType.DMA((3,)),
            pltpu.SemaphoreType.DMA((parts,)),
            out_scratch[1],
            pltpu.SemaphoreType.DMA,
        ],
        out_shape=[one_block(length, wide)] * 2 + [one_block(length, inner)],
        cost_estimate=pl.CostEstimate(
            flops=2 * length * wide * RING * 4 * inner, bytes_accessed=10**7, transcendentals=0
        ),
        compiler_params=pltpu.CompilerParams(vmem_limit_bytes=50 * 2**20),
        name="attention",
    )(
        *[held[k] for k in range(RING)],
        *own,
        other,
        *out_weights,
        bias,
    )
    rest = pl.pallas_call(
        out_rest_kernel,
        in_specs=[ANY] * 4,
        out_specs=IN_VMEM,
        scratch_shapes=out_scratch
        + [pltpu.VMEM((length, inner), jnp.bfloat16), pltpu.SemaphoreType.DMA],
        out_shape=rest_blocks(length, wide),
        cost_estimate=pl.CostEstimate(
            flops=2 * length * inner * wide * (RING - 2),
            bytes_accessed=4 * 10**6,
            transcendentals=0,
        ),
        compiler_params=pltpu.CompilerParams(vmem_limit_bytes=52 * 2**20),
        name="out_rest",
    )(attended, *out_weights)
    return first, second, rest


FIRST = (0, 1, 7)
SECOND = (2, 6)
THIRD = (3, 5)
LAST = (4,)


def gate_copies(owners, blocks, gate_ref, up_ref, other_ref, x_ref, w_ref, x_sem, w_sem):
    wide, hidden = x_ref.shape[2], gate_ref.shape[1]
    ring_at = lax.axis_index("ma_0")
    copies = []
    for k, (owner, block) in enumerate(zip(owners, blocks)):
        slot = lax.rem(ring_at + owner, RING)
        row = pl.ds(pl.multiple_of(slot * wide, wide), wide)
        copies.append(pltpu.make_async_copy(block, x_ref.at[k], x_sem.at[k]))
        sources = [
            gate_ref.at[row, :],
            up_ref.at[row, :],
            other_ref.at[slot, pl.ds(0, wide), :],
            other_ref.at[slot, pl.ds(wide, wide), :],
        ]
        for n, source in enumerate(sources):
            copies.append(
                pltpu.make_async_copy(
                    source, w_ref.at[k, :, pl.ds(n * hidden, hidden)], w_sem.at[k, n]
                )
            )
    return copies


def gate_kernel(owners, more, *refs):
    count = len(owners)
    blocks = refs[:count]
    gate_ref, up_ref, other_ref = refs[count : count + 3]
    refs = refs[count + 3 :]
    if more:
        acc_in_ref, squares_in_ref, refs = refs[0], refs[1], refs[2:]
    acc_ref, squares_ref, x_ref, w_ref, x_sem, w_sem, sum_sem = refs
    length = acc_ref.shape[0]
    copies = gate_copies(owners, blocks, gate_ref, up_ref, other_ref, x_ref, w_ref, x_sem, w_sem)
    if more:
        copies.append(pltpu.make_async_copy(squares_in_ref, squares_ref, sum_sem.at[0]))
        copies.append(pltpu.make_async_copy(acc_in_ref, acc_ref, sum_sem.at[1]))
    for copy in copies:
        copy.start()
    if not more:
        acc_ref[...] = jnp.zeros_like(acc_ref)
        squares_ref[...] = jnp.zeros_like(squares_ref)
    for copy in copies:
        copy.wait()

    def add_block(k, unused):
        squares_ref[...] += x_ref[k, length : length + 8, :length].astype(jnp.float32)
        acc_ref[...] += dot(x_ref[k, :length, :], w_ref[k])
        return unused

    lax.fori_loop(0, count, add_block, 0)


def hidden_kernel(width, *refs):
    count = len(LAST)
    blocks = refs[:count]
    gate_ref, up_ref, other_ref, acc_in_ref, squares_in_ref = refs[count : count + 5]
    hidden_ref, x_ref, w_ref, x_sem, w_sem, sum_sem, acc_ref, squares_ref = refs[count + 5 :]
    size = gate_ref.shape[1]
    length = hidden_ref.shape[0]
    copies = gate_copies(LAST, blocks, gate_ref, up_ref, other_ref, x_ref, w_ref, x_sem, w_sem)
    copies.append(pltpu.make_async_copy(squares_in_ref, squares_ref, sum_sem.at[0]))
    copies.append(pltpu.make_async_copy(acc_in_ref, acc_ref, sum_sem.at[1]))
    for copy in copies:
        copy.start()
    for copy in copies:
        copy.wait()
    rows = x_ref[0, :length, :]
    squares = squares_ref[0:1, :] + x_ref[0, length : length + 1, :length].astype(jnp.float32)
    scale = as_column(lax.rsqrt(squares / width + epsilon))
    for k in range(2):
        sums = []
        for n in (2 * k, 2 * k + 1):
            at = slice(n * size, (n + 1) * size)
            sums.append((acc_ref[:, at] + dot(rows, w_ref[0, :, at])) * scale)
        hidden_ref[:, k * size : (k + 1) * size] = (
            jax.nn.gelu(sums[0], approximate=True) * sums[1]
        ).astype(jnp.bfloat16)


def down_copies(owners, down_ref, other_ref, d_ref, d_sem):
    ring_at, pair_at = lax.axis_index("ma_0"), lax.axis_index("ma_1")
    part = d_ref.shape[2]
    size = down_ref.shape[0]
    copies = []
    for j, owner in enumerate(owners):
        slot = lax.rem(ring_at + owner, RING)
        column = pl.multiple_of((slot * 2 + pair_at) * part, part)
        sources = [down_ref.at[:, pl.ds(column, part)]]
        sources += [other_ref.at[slot, pl.ds(n * size, size), :] for n in (4, 6, 5)]
        for n, source in enumerate(sources):
            copies.append(
                pltpu.make_async_copy(source, d_ref.at[j, pl.ds(n * size, size), :], d_sem.at[j, n])
            )
    return copies


def down_kernel(owners, mine_ref, theirs_ref, down_ref, other_ref, *refs):
    *out_refs, h_ref, d_ref, h_sem, d_sem = refs
    copies = [
        pltpu.make_async_copy(ref, h_ref.at[k], h_sem.at[k])
        for k, ref in enumerate((mine_ref, theirs_ref))
    ] + down_copies(owners, down_ref, other_ref, d_ref, d_sem)
    for copy in copies:
        copy.start()
    for copy in copies:
        copy.wait()
    rows = h_ref.shape[2]

    def block(j):
        product = dot(h_ref[0], d_ref[j, :rows, :]) + dot(h_ref[1], d_ref[j, rows:, :])
        return product.astype(jnp.bfloat16)

    if len(out_refs) > 1:
        for j, out_ref in enumerate(out_refs):
            out_ref[...] = block(j)
        return

    def store(j, unused):
        out_refs[0][j] = block(j)
        return unused

    lax.fori_loop(0, len(owners), store, 0)


def feed_forward(held, gate, up, down, other):
    rows, wide = held[0].shape
    hidden = gate.shape[1]
    length = rows - 8
    part = wide // 2
    sums = [
        jax.ShapeDtypeStruct((length, 4 * hidden), jnp.float32),
        jax.ShapeDtypeStruct((8, length), jnp.float32),
    ]

    def scratch(count):
        return [
            pltpu.VMEM((count, rows, wide), jnp.bfloat16),
            pltpu.VMEM((count, wide, 4 * hidden), jnp.bfloat16),
            pltpu.SemaphoreType.DMA((count,)),
            pltpu.SemaphoreType.DMA((count, 4)),
            pltpu.SemaphoreType.DMA((2,)),
        ]

    def cost(count, extra=0):
        return pl.CostEstimate(
            flops=2 * length * wide * 4 * hidden * count + extra,
            bytes_accessed=10**6 * (count + 1),
            transcendentals=0,
        )

    def gate_sums(owners, before):
        return pl.pallas_call(
            functools.partial(gate_kernel, owners, bool(before)),
            in_specs=[ANY] * (len(owners) + 3 + len(before)),
            out_specs=[IN_VMEM] * 2,
            scratch_shapes=scratch(len(owners)),
            out_shape=sums,
            compiler_params=pltpu.CompilerParams(vmem_limit_bytes=50 * 2**20),
            cost_estimate=cost(len(owners)),
        )(*[held[k] for k in owners], gate, up, other, *before)

    before = gate_sums(FIRST, ())
    before = gate_sums(SECOND, before)
    before = gate_sums(THIRD, before)
    mine = pl.pallas_call(
        functools.partial(hidden_kernel, float(wide * RING)),
        in_specs=[ANY] * (len(LAST) + 5),
        out_specs=IN_VMEM,
        scratch_shapes=scratch(len(LAST)) + [pltpu.VMEM(s.shape, s.dtype) for s in sums],
        out_shape=jax.ShapeDtypeStruct((length, 2 * hidden), jnp.bfloat16),
        compiler_params=pltpu.CompilerParams(vmem_limit_bytes=52 * 2**20),
        cost_estimate=cost(1),
        name="hidden",
    )(*[held[k] for k in LAST], gate, up, other, *before)
    theirs = lax.ppermute(mine, "ma_1", SWAP)

    def down_blocks(owners, shapes):
        return pl.pallas_call(
            functools.partial(down_kernel, owners),
            in_specs=[ANY] * 4,
            out_specs=[IN_VMEM] * len(shapes),
            scratch_shapes=[
                pltpu.VMEM((2, length, 2 * hidden), jnp.bfloat16),
                pltpu.VMEM((len(owners), 4 * hidden, part), jnp.bfloat16),
                pltpu.SemaphoreType.DMA((2,)),
                pltpu.SemaphoreType.DMA((len(owners), 4)),
            ],
            out_shape=shapes,
            compiler_params=pltpu.CompilerParams(vmem_limit_bytes=52 * 2**20),
            cost_estimate=cost(1),
        )(mine, theirs, down, other)

    first, second = down_blocks(SEND[:2], [one_block(length, part)] * 2)
    (rest,) = down_blocks(SEND[2:], [rest_blocks(length, part)])
    return first, second, rest


def spread(values, gain):
    rows, width = values.shape
    as_float = values.astype(jnp.float32)
    squares = jnp.sum(as_float * as_float, axis=1)
    gained = (as_float * gain.astype(jnp.float32)).astype(jnp.bfloat16)
    line = jnp.concatenate([squares, jnp.zeros((width - rows,), jnp.float32)])
    tail = jnp.broadcast_to(line.astype(jnp.bfloat16)[None], (8, width))
    block = jnp.concatenate([gained, tail], axis=0)
    return ring_gather(block)


def layer(
    tokens,
    attn_gain,
    query_weight,
    key_weight,
    value_projection_matrix,
    attention_output_matrix,
    bucket_bias_matrix,
    ffn_gain,
    gate_weight,
    up_weight,
    down_projection_weight,
):
    sequences, length, part = tokens.shape
    copy_at = lax.axis_index("ba")
    copies = lax.axis_size("ba")
    token_rows = tokens.reshape(length, part)

    gains = jnp.concatenate(
        [attn_gain[None], ffn_gain[None], jnp.zeros((6, part), jnp.bfloat16)], axis=0
    )
    mine = jnp.concatenate([token_rows, gains], axis=0)
    theirs = lax.ppermute(mine, "ma_1", SWAP)

    half_rows = query_weight.shape[0]
    depth = half_rows // copies
    share = [
        lax.dynamic_slice_in_dim(w, copy_at * depth, depth, 0)
        for w in (query_weight, key_weight, value_projection_matrix)
    ]
    first_share = lax.ppermute(jnp.concatenate(share, axis=1), "row", SWAP)
    other_first = lax.all_gather(first_share, "ba", axis=0, tiled=True)
    gate_depth = gate_weight.shape[0] // copies
    gate_share = [
        lax.dynamic_slice_in_dim(w, copy_at * gate_depth, gate_depth, 0)
        for w in (gate_weight, up_weight)
    ]
    down_width = down_projection_weight.shape[1] // copies
    pair_at = lax.axis_index("ma_1")

    def down_share(pair):
        at = copy_at * down_width + pair * part
        return lax.dynamic_slice_in_dim(down_projection_weight, at, part, 1)

    wide = pair_order(mine, theirs, 1)
    wide_tokens = wide[:length]
    wide_attn_gain = wide[length]
    wide_ffn_gain = wide[length + 1]

    held = spread(wide_tokens, wide_attn_gain)
    core_width = attention_output_matrix.shape[1] // 2
    core_out = lax.dynamic_slice_in_dim(
        attention_output_matrix, jnp.mod(copy_at, 2) * core_width, core_width, 1
    )
    core_out = lax.ppermute(tied(core_out, held[1]), "row", SWAP)
    cores = [(k, k ^ 1) for k in range(copies)]
    other_core_out = lax.ppermute(core_out, "ba", cores)
    pair_share = tied(down_share(1 - pair_at), held[1])
    pair_share = lax.ppermute(pair_share, "ma_1", SWAP)
    pair_share = tied(pair_share, held[3])
    same_share = down_share(pair_at)
    row_share = jnp.concatenate([*gate_share, same_share, pair_share], axis=0)
    row_share = lax.ppermute(row_share, "row", SWAP)
    out_blocks = attention(
        held,
        position_bias(bucket_bias_matrix, length),
        (query_weight, key_weight, value_projection_matrix),
        other_first,
        (attention_output_matrix, core_out, other_core_out),
    )
    row_share = tied(row_share, out_blocks[0])
    second_share = jnp.concatenate([row_share, pair_share], axis=0)
    other_second = lax.all_gather(second_share, "ba", axis=0, tiled=False)
    summed = ring_sum(*out_blocks).astype(jnp.bfloat16)
    partner = lax.ppermute(summed, "ma_1", SWAP)
    attn_out = summed.astype(jnp.float32) + partner.astype(jnp.float32)
    residual = (wide_tokens.astype(jnp.float32) + attn_out).astype(jnp.bfloat16)
    first = lax.axis_index("ma_1") == 0
    own_residual = jnp.where(first, residual[:, :part], residual[:, part:])

    held = spread(residual, wide_ffn_gain)
    summed = ring_sum(
        *feed_forward(held, gate_weight, up_weight, down_projection_weight, other_second),
    )
    encoded = own_residual.astype(jnp.float32) + summed
    return encoded.astype(jnp.bfloat16).reshape(sequences, length, part)


def solution(mesh):
    split = Mesh(
        mesh.devices.reshape(mesh.shape["ba"], RING, 2, mesh.shape["row"]),
        ("ba", "ma_0", "ma_1", "row"),
    )
    return jax.shard_map(
        layer,
        mesh=split,
        in_specs=(
            P(("ba", "row"), None, MA),
            P(MA),
            P("row", MA),
            P("row", MA),
            P("row", MA),
            P(MA, "row"),
            P(None, MA),
            P(MA),
            P(None, MA_ROW),
            P(None, MA_ROW),
            P(MA_ROW, None),
        ),
        out_specs=P(("ba", "row"), None, MA),
        check_vma=False,
    )
```
